256 devices in a mesh: epoch: 64 (over y, z, x_lo), blend: 4 (over x_hi, core).
Axes of the slice: x: 4 (x_hi: 2, x_lo: 2; x = x_hi * 2 + x_lo), y: 4, z: 8, core: 2. Of those that a mesh axis runs over, the one named last changes fastest.
Arguments:
- models: float32 [4, 128, 6, 4096], P('blend', 'epoch'), may hold values from -6 to 6
- observed: bfloat16 [64, 512, 4096], P('epoch', 'blend'), may hold values from -6 to 6
- weights: float32 [64, 512], P('epoch', 'blend'), may hold values from 0.5 to 2
- coverage: int32 [64, 512], P('epoch', 'blend'), may hold values from 0 to 1, as said below
- offsets: int32 [64, 512, 2], P('epoch', 'blend'), may hold values from 0 to 63
- counts: int32 [4, 128], P('blend', 'epoch'), may hold values from 1 to 64, as said below
- psf_y: bfloat16 [64, 4096], P('epoch'), may hold values from -0.75 to 0.75
- resample_y: bfloat16 [64, 4096], P('epoch'), may hold values from -0.75 to 0.75
- psf_x: bfloat16 [64, 4096], P('epoch'), may hold values from -0.75 to 0.75
- resample_x: bfloat16 [64, 4096], P('epoch'), may hold values from -0.75 to 0.75
Outputs:
- updated: float32 [4, 128, 6, 4096], P('blend', 'epoch')
The draws below stay inside these ranges and needn't reach their ends.
Inputs may be any that keep to these rules, and one draw needn't show every extreme that they name: `coverage`: every blend is seen by one epoch or more. counts of blend b is the sum of coverage over all epochs for b.
All inputs are finite; a program needn't handle non-finite values.
Results may differ from the reference program's by a relative error of at most 0.0017.
Values may be sent and summed in bfloat16 or wider, within the bound.
A program may use at most 128 MiB of HBM per device.

```python
import math
import jax
import jax.numpy as jnp
from jax import lax

CUT = 64
BANDS = 6
PIX2 = 4096
E = 64
BLEND_GRP = 128
B = 512
N_BLEND = 4


def coverage_table(key):
    inner = jax.random.fold_in(key, 11)
    chance = jax.random.randint(jax.random.fold_in(inner, 1), (B,), 10, 95)
    rolled = jax.random.randint(jax.random.fold_in(inner, 2), (E, B), 0, 100)
    seen = rolled < chance[None, :]
    forced = jnp.arange(E, dtype=jnp.int32)[:, None] == jnp.arange(B, dtype=jnp.int32)[None, :] % E
    return jnp.logical_or(seen, forced).astype(jnp.int32)


def draw_coverage(key, part):
    return coverage_table(key)


def draw_counts(key, part):
    return jnp.sum(coverage_table(key), axis=0).astype(jnp.int32).reshape(N_BLEND, BLEND_GRP)


def place_ends(values, rng, smallest, top_value):
    longest = values.shape.index(max(values.shape))
    spots = []
    for shift in (0, 1):
        where = [jax.random.randint(jax.random.fold_in(rng, axis), (), 0, length) for axis, length in enumerate(values.shape)]
        where[longest] = (where[longest] + shift) % values.shape[longest]
        spots.append(tuple(where))
    return values.at[spots[0]].set(smallest).at[spots[1]].set(top_value)


def steps_of(stream_key, extent, pieces, smallest, largest):
    gain = 1.0
    for dim, shards_of in pieces:
        heights = jax.random.uniform(jax.random.fold_in(jax.random.fold_in(stream_key, 6), dim), (shards_of,), jnp.float32, smallest / len(pieces), largest / len(pieces))
        gain = gain * jnp.repeat(jnp.exp(heights), extent[dim] // shards_of).reshape((-1,) + (1,) * (len(extent) - 1 - dim))
    return gain


def centred(own_key, dims, deviation, reach, split=(), held_as=jnp.bfloat16):
    array = jax.random.normal(own_key, dims, jnp.float32) * deviation
    if len(split) > 0:
        array = steps_of(own_key, dims, split, -0.22, 0.18) * array
    return jnp.clip(array, min=-reach, max=reach).astype(held_as)


def setup_inputs(seed: int = 0) -> dict:
    arg_keys = jax.random.split(jax.random.key(seed), 11)
    return {
        "models": centred(arg_keys[0], (N_BLEND, BLEND_GRP, BANDS, PIX2), 1.0, 6.0, ((0, 4), (1, 64)), jnp.float32),
        "observed": centred(arg_keys[1], (E, B, PIX2), 1.0, 6.0, ((0, 64), (1, 4))),
        "weights": jnp.clip(jnp.exp(math.log(2.0) - 1.3862944 * jax.random.uniform(arg_keys[2], (E, B), jnp.float32) ** steps_of(arg_keys[2], (E, B), ((0, 64), (1, 4)), -0.2, 0.2)), 0.5, 2.0),
        "coverage": draw_coverage(jax.random.fold_in(arg_keys[10], 71), 0),
        "offsets": place_ends(jax.random.randint(arg_keys[4], (E, B, 2), 0, CUT), jax.random.fold_in(arg_keys[4], 1), 0, CUT - 1).astype(jnp.int32),
        "counts": draw_counts(jax.random.fold_in(arg_keys[10], 71), 0),
        "psf_y": centred(arg_keys[6], (E, PIX2), CUT ** -0.5, 0.75, ((0, 64),)),
        "resample_y": centred(arg_keys[7], (E, PIX2), CUT ** -0.5, 0.75, ((0, 64),)),
        "psf_x": centred(arg_keys[8], (E, PIX2), CUT ** -0.5, 0.75, ((0, 64),)),
        "resample_x": centred(arg_keys[9], (E, PIX2), CUT ** -0.5, 0.75, ((0, 64),)),
    }


step_size = 0.5


def roll_forward(image, down, across):
    side = image.shape[0]
    doubled = jnp.concatenate([image, image], axis=0)
    rows = lax.dynamic_slice_in_dim(doubled, down, side, 0)
    doubled = jnp.concatenate([rows, rows], axis=1)
    return lax.dynamic_slice_in_dim(doubled, across, side, 1)


def one_epoch(model_low, observed, scale, offsets, left, right, band):
    side = left.shape[0]
    count = observed.shape[0]
    chosen = lax.dynamic_index_in_dim(model_low, band, 1, keepdims=False)
    shifted = jax.vmap(roll_forward)(chosen, offsets[:, 0], offsets[:, 1])
    blurred = jnp.einsum('ij,bjk->bik', left.astype(jnp.float32), shifted.astype(jnp.float32)).astype(jnp.bfloat16)
    predicted = jnp.einsum('bik,lk->bil', blurred.astype(jnp.float32), right.astype(jnp.float32))
    target = observed.reshape(count, side, side).astype(jnp.float32)
    misfit = (scale[:, None, None] * (predicted - target)).astype(jnp.bfloat16)
    back = jnp.einsum('ji,bjk->bik', left.astype(jnp.float32), misfit.astype(jnp.float32)).astype(jnp.bfloat16)
    term = jnp.einsum('bik,kl->bil', back.astype(jnp.float32), right.astype(jnp.float32))
    return jax.vmap(roll_forward)(term, side - offsets[:, 0], side - offsets[:, 1])


def reference(models, observed, weights, coverage, offsets, counts, psf_y, resample_y, psf_x, resample_x):
    flat = models.reshape(B, BANDS, CUT, CUT)
    model_low = flat.astype(jnp.bfloat16)
    lefts = jnp.einsum('eij,ejk->eik', psf_y.reshape(E, CUT, CUT).astype(jnp.float32), resample_y.reshape(E, CUT, CUT).astype(jnp.float32)).astype(jnp.bfloat16)
    rights = jnp.einsum('eij,ejk->eik', psf_x.reshape(E, CUT, CUT).astype(jnp.float32), resample_x.reshape(E, CUT, CUT).astype(jnp.float32)).astype(jnp.bfloat16)
    scale = weights * coverage.astype(jnp.float32)

    def advance(gradient, inputs):
        epoch_id, seen, weight_row, offset_row, left, right = inputs
        band = (epoch_id * BANDS) // E
        term = one_epoch(model_low, seen, weight_row, offset_row, left, right, band)
        current = lax.dynamic_index_in_dim(gradient, band, 0, keepdims=False)
        gradient = lax.dynamic_update_index_in_dim(gradient, current + term, band, 0)
        return gradient, None

    start_grad = jnp.zeros((BANDS, B, CUT, CUT), jnp.float32)
    epochs = jnp.arange(E, dtype=jnp.int32)
    gradient, _ = lax.scan(advance, start_grad, (epochs, observed, scale, offsets, lefts, rights))
    gradient = gradient.transpose(1, 0, 2, 3).reshape(B, BANDS, PIX2)
    divisor = counts.reshape(B).astype(jnp.float32)[:, None, None]
    updated = models.reshape(B, BANDS, PIX2) - step_size * gradient / divisor
    return updated.reshape(N_BLEND, BLEND_GRP, BANDS, PIX2)
```

```python
import functools

import jax
import jax.numpy as jnp
from jax import lax
from jax.experimental import pallas as pl
from jax.experimental.pallas import tpu as pltpu
from jax.sharding import PartitionSpec as P

CUT = 64
BANDS = 6
PIX2 = 4096
E = 64
NY, NZ = 4, 8
step_size = 0.5
MESH = pl.DeviceIdType.MESH
F32, BF16 = jnp.float32, jnp.bfloat16


def band_of(epoch):
    return epoch * BANDS // E


STRADDLERS = [
    (y, z) for y in range(NY) for z in range(NZ) if band_of((y * NZ + z) * 2) != band_of((y * NZ + z) * 2 + 1)
]


def kernel(
    models, obs_hbm, weights, coverage, offs, counts, psf_y, res_y, psf_x, res_x, out,
    obs_v, obs_st, obs_in, models_low, mod_in, term_out, term_out2, term_in, term_in2,
    mats, mats_in, tab_a, tab_at, tab_r, fold, rows_f, wide, spread,
    scale_v, scale_in, offs_in, off_own, off_par, sc_own, sc_par,
    in_s, in_r, in2_s, in2_r, obs_s, obs_r, t_s, t_r, t2_s, t2_r, small_s, small_r, local,
):
    me = lax.axis_index("epoch")
    x = lax.rem(me, 2)
    z = lax.rem(lax.div(me, 2), NZ)
    y = lax.div(me, 2 * NZ)
    partner = me + 1 - 2 * x

    def device(yy, zz):
        return (yy * NZ + zz) * 2 + x

    def place(ky, kz):
        return lax.rem(y + ky, NY), lax.rem(z + kz, NZ)

    relative = [(ky, kz) for kz in (4, 3, 5, 2, 6, 1, 7, 0) for ky in (2, 1, 3, 0)]
    others = [r for r in relative if r != (0, 0)]

    def remote(src, dst, send, recv, target):
        return pltpu.make_async_remote_copy(
            src_ref=src, dst_ref=dst, send_sem=send, recv_sem=recv, device_id={"epoch": target}, device_id_type=MESH
        )

    barrier = pltpu.get_barrier_semaphore()
    pl.semaphore_signal(barrier, inc=1, device_id={"epoch": partner}, device_id_type=MESH)
    for ky, kz in others:
        pl.semaphore_signal(barrier, inc=1, device_id={"epoch": device(*place(ky, kz))}, device_id_type=MESH)

    load_obs = pltpu.make_async_copy(obs_hbm, obs_v, local.at[0])
    load_obs.start()
    load_off = pltpu.make_async_copy(offs, off_own, local.at[1])
    load_off.start()
    scale_v[...] = weights[...] * coverage[...].astype(F32)

    straddle = jnp.int32(0)
    straddle_id = jnp.int32(0)
    for i, (ys, zs) in enumerate(STRADDLERS):
        hit = jnp.where(jnp.logical_and(y == ys, z == zs), 1, 0).astype(jnp.int32)
        straddle = straddle + hit
        straddle_id = straddle_id + i * hit

    lane = lax.broadcasted_iota(jnp.int32, (CUT, 128), 1)
    row = lax.broadcasted_iota(jnp.int32, (CUT, 128), 0)
    low = lane < CUT
    low_half = low[:32]
    even = lax.rem(row, 2) == 0
    mask_lo = jnp.where(low, 1.0, 0.0).astype(BF16)
    mask_hi = jnp.where(low, 0.0, 1.0).astype(BF16)

    def swap(v):
        turned = pltpu.roll(v, CUT, 1)
        up = pltpu.roll(turned, CUT - 1, 0)
        down = pltpu.roll(turned, 1, 0)
        return jnp.where(low, jnp.where(even, v, down), jnp.where(even, up, v))

    def unfold(ref):
        v = ref[...].astype(F32)
        for k in range(32):
            fold[k : k + 1, :] = v[:, k * 128 : (k + 1) * 128]
        top = fold[...]
        return top, pltpu.roll(top, CUT, 1)

    def natural(ref):
        top, bottom = unfold(ref)
        rows_f[pl.ds(0, 32, stride=2), :] = top
        rows_f[pl.ds(1, 32, stride=2), :] = bottom
        return rows_f[...]

    def doubled(v):
        return jnp.where(low, v, pltpu.roll(v, CUT, 1))

    top, bottom = unfold(psf_y)
    first = jnp.concatenate([top, bottom], axis=0)[:, :CUT].astype(BF16)
    second = doubled(natural(res_y)).astype(BF16)
    mats[0] = jnp.dot(first, second, preferred_element_type=F32).astype(BF16)
    first = natural(psf_x)[:, :CUT].astype(BF16)
    second = doubled(natural(res_x)).astype(BF16)
    mats[1] = jnp.dot(first, second, preferred_element_type=F32).astype(BF16)

    for c in range(BANDS):
        models_low[c] = swap(models[c]).astype(BF16)

    def tables(slot, source):
        left = source[0].astype(F32)
        right = source[1].astype(F32)
        wide[...] = jnp.concatenate([left, left], axis=0).T

        def one(d, carry):
            tab_a[slot, d] = pltpu.roll(left, d, 1).astype(BF16)
            tab_at[slot, d] = wide[pl.ds(CUT - d, CUT), :].astype(BF16)
            tab_r[slot, d] = pltpu.roll(right, d, 1).astype(BF16)
            return carry

        lax.fori_loop(0, CUT, one, 0, unroll=4)

    load_obs.wait()

    def relayout(m, carry):
        spread[...] = obs_v[m].astype(F32)
        yy = lax.div(m, 4)
        z2 = 2 * lax.rem(m, 4)
        for s in range(4):
            f0 = spread[pl.ds(2 * s, 32, stride=8), :]
            f1 = spread[pl.ds(2 * s + 1, 32, stride=8), :]
            top = jnp.where(low_half, f0, pltpu.roll(f1, CUT, 1))
            bottom = jnp.where(low_half, pltpu.roll(f0, CUT, 1), f1)
            obs_st[s % 2, z2 + s // 2, yy] = jnp.concatenate([top, bottom], axis=0).astype(BF16)
        return carry

    lax.fori_loop(0, 16, relayout, 0)

    load_off.wait()
    load_scale = pltpu.make_async_copy(scale_v, sc_own, local.at[2])
    load_scale.start()
    load_scale.wait()

    pl.semaphore_wait(barrier, 32)

    send_mats = remote(mats, mats_in, small_s.at[0], small_r.at[0], partner)
    send_off = remote(offs, offs_in, small_s.at[1], small_r.at[1], partner)
    send_scale = remote(scale_v, scale_in, small_s.at[2], small_r.at[2], partner)
    send_mats.start()
    send_off.start()
    send_scale.start()

    def obs_copy(g):
        zz = lax.rem(z + far_first(g), NZ)
        return remote(obs_st.at[1 - x, zz], obs_in.at[zz], obs_s.at[g], obs_r.at[g], partner)

    def far_first(g):
        return 4 + lax.div(g + 1, 2) * (1 - 2 * lax.rem(g, 2))

    for g in range(8):
        obs_copy(jnp.int32(g)).start()

    def model_copy(ky, kz):
        yy, zz = place(ky, kz)
        band = lax.div((yy * NZ + zz) * 2 * BANDS, E)
        return remote(
            models_low.at[band], mod_in.at[0, z, y], in_s.at[zz * NY + yy], in_r.at[z * NY + y], device(yy, zz)
        )

    for ky, kz in others:
        model_copy(ky, kz).start()
    for i, (ys, zs) in enumerate(STRADDLERS):
        band = band_of((ys * NZ + zs) * 2 + 1)
        here = jnp.logical_and(y == ys, z == zs)

        @pl.when(jnp.logical_not(here))
        def _():
            remote(
                models_low.at[band], mod_in.at[1, z, y], in2_s.at[i], in2_r.at[z * NY + y], device(ys, zs)
            ).start()

        @pl.when(here)
        def _():
            mod_in[1, z, y] = models_low[band]

    mod_in[0, z, y] = models_low[lax.div((y * NZ + z) * 2 * BANDS, E)]

    tables(0, mats)
    send_mats.wait_recv()
    tables(1, mats_in)
    send_off.wait_recv()
    send_scale.wait_recv()
    load_off = pltpu.make_async_copy(offs_in, off_par, local.at[3])
    load_scale = pltpu.make_async_copy(scale_in, sc_par, local.at[4])
    load_off.start()
    load_scale.start()
    load_off.wait()
    load_scale.wait()

    slot_own = straddle * x
    slot_par = straddle * (1 - x)
    own_first = slot_own == 0
    par_first = slot_par == 0
    offsets = (off_own, off_par)
    scales = (sc_own, sc_par)

    def term_copy(yy, zz):
        return remote(
            term_out.at[zz, yy], term_in.at[z, y], t_s.at[zz * NY + yy], t_r.at[z * NY + y], device(yy, zz)
        )

    def term2_copy(yy, zz):
        return remote(
            term_out2.at[zz, yy], term_in2.at[straddle_id], t2_s.at[zz * NY + yy], t2_r.at[straddle_id], device(yy, zz)
        )

    def split(v):
        return jnp.concatenate([v * mask_lo, v * mask_hi], axis=0)

    def group(g, carry):
        zz = lax.rem(z + far_first(g), NZ)
        obs_copy(g).wait_recv()
        units = []
        for ky in (2, 1, 3, 0):
            yy = lax.rem(y + ky, NY)

            def arrive():
                slot = zz * NY + yy
                remote(models_low.at[0], mod_in.at[0, zz, yy], in_s.at[slot], in_r.at[slot], partner).wait_recv()

                @pl.when(straddle == 1)
                def _():
                    remote(models_low.at[0], mod_in.at[1, zz, yy], in_s.at[slot], in2_r.at[slot], partner).wait_recv()

            if ky == 0:
                pl.when(g < 7)(arrive)
            else:
                arrive()
            for e in range(2):
                units.append((yy, e))
        state = []
        for yy, e in units:
            b = 2 * ((yy * NZ + zz) * 2 + x)
            dy0, dx0 = offsets[e][0, b], offsets[e][1, b]
            dy1, dx1 = offsets[e][0, b + 1], offsets[e][1, b + 1]
            left = tab_a[e, dy0] * mask_lo + tab_a[e, dy1] * mask_hi
            image = mod_in[slot_own if e == 0 else slot_par, zz, yy]
            blurred = jnp.dot(left, split(image), preferred_element_type=F32).astype(BF16)
            state.append([yy, e, b, dy0, dy1, dx0, dx1, blurred])
        for s in state:
            yy, e, b, dy0, dy1, dx0, dx1, blurred = s
            right = jnp.concatenate([tab_r[e, dx0] * mask_lo, tab_r[e, dx1] * mask_hi], axis=0)
            predicted = lax.dot_general(blurred, right, (((1,), (1,)), ((), ())), preferred_element_type=F32)
            seen = (obs_st[x, zz, yy] if e == 0 else obs_in[zz, yy]).astype(F32)
            scale = jnp.where(low[:1], scales[e][0, b], scales[e][0, b + 1])
            s.append((scale * (predicted - seen)).astype(BF16))
        for s in state:
            yy, e, b, dy0, dy1, dx0, dx1, blurred, misfit = s
            left_t = tab_at[e, dy0] * mask_lo + tab_at[e, dy1] * mask_hi
            s.append(jnp.dot(left_t, split(misfit), preferred_element_type=F32).astype(BF16))
        terms = {}
        for s in state:
            yy, e, b, dy0, dy1, dx0, dx1, blurred, misfit, back = s
            right = jnp.concatenate([tab_r[e, dx0] * mask_lo, tab_r[e, dx1] * mask_hi], axis=0)
            terms.setdefault(len(terms) if e == 0 else len(terms) - 1, [yy]).append(
                jnp.dot(back, right, preferred_element_type=F32)
            )
        for yy, own, par in terms.values():
            zero = jnp.zeros_like(own)
            term_out[zz, yy] = (jnp.where(own_first, own, zero) + jnp.where(par_first, par, zero)).astype(BF16)
            term_out2[zz, yy] = (jnp.where(own_first, zero, own) + jnp.where(par_first, zero, par)).astype(BF16)
        for ky in (2, 1, 3, 0):
            yy = lax.rem(y + ky, NY)

            def ship():
                term_copy(yy, zz).start()

                @pl.when(straddle == 1)
                def _():
                    term2_copy(yy, zz).start()

            if ky == 0:
                pl.when(g < 7)(ship)
            else:
                ship()
        return carry

    lax.fori_loop(0, 8, group, 0)

    term_in[z, y] = term_out[z, y]

    @pl.when(straddle == 1)
    def _():
        term_in2[straddle_id] = term_out2[z, y]

    for ky, kz in others:
        yy, zz = place(ky, kz)
        slot = zz * NY + yy
        remote(term_out.at[zz, yy], term_in.at[zz, yy], t_s.at[slot], t_r.at[slot], partner).wait_recv()
    for i, (ys, zs) in enumerate(STRADDLERS):

        @pl.when(jnp.logical_not(jnp.logical_and(y == ys, z == zs)))
        def _():
            remote(term_out2.at[0, 0], term_in2.at[i], t2_s.at[0], t2_r.at[i], partner).wait_recv()

    seen_by = jnp.where(even, counts[0, 0].astype(F32), counts[0, 1].astype(F32))
    factor = step_size / seen_by
    for c in range(BANDS):
        total = jnp.zeros((CUT, 128), F32)
        for yy in range(NY):
            for zz in range(NZ):
                if band_of((yy * NZ + zz) * 2) == c:
                    total = total + term_in[zz, yy].astype(F32)
        for i, (ys, zs) in enumerate(STRADDLERS):
            if band_of((ys * NZ + zs) * 2 + 1) == c:
                total = total + term_in2[i].astype(F32)
        out[c] = models[c] - factor * swap(total)

    send_mats.wait_send()
    send_off.wait_send()
    send_scale.wait_send()
    for g in range(8):
        obs_copy(jnp.int32(g)).wait_send()
    for ky, kz in others:
        model_copy(ky, kz).wait_send()
        yy, zz = place(ky, kz)
        term_copy(yy, zz).wait_send()

        @pl.when(straddle == 1)
        def _():
            term2_copy(yy, zz).wait_send()

    for i, (ys, zs) in enumerate(STRADDLERS):

        @pl.when(jnp.logical_not(jnp.logical_and(y == ys, z == zs)))
        def _():
            remote(models_low.at[0], mod_in.at[1, z, y], in2_s.at[i], in2_r.at[0], partner).wait_send()


def on_device(
    models, observed, weights, coverage, offsets, counts, psf_y, resample_y, psf_x, resample_x
):
    pair_models = models[0].reshape(2, BANDS, 32, 128).transpose(1, 2, 0, 3).reshape(BANDS, CUT, 128)
    blocks = observed[0].reshape(16, 8, 32, 128).transpose(0, 2, 1, 3).reshape(16, 256, 128)
    vmem = pl.BlockSpec(memory_space=pltpu.VMEM)
    dma = pltpu.SemaphoreType.DMA
    updated = pl.pallas_call(
        kernel,
        out_shape=jax.ShapeDtypeStruct((BANDS, CUT, 128), F32),
        in_specs=[
            vmem, pl.BlockSpec(memory_space=pl.ANY), vmem, vmem, vmem, pl.BlockSpec(memory_space=pltpu.SMEM),
            vmem, vmem, vmem, vmem,
        ],
        out_specs=vmem,
        scratch_shapes=[
            pltpu.VMEM((16, 256, 128), BF16),
            pltpu.VMEM((2, NZ, NY, CUT, 128), BF16),
            pltpu.VMEM((NZ, NY, CUT, 128), BF16),
            pltpu.VMEM((BANDS, CUT, 128), BF16),
            pltpu.VMEM((2, NZ, NY, CUT, 128), BF16),
            pltpu.VMEM((NZ, NY, CUT, 128), BF16),
            pltpu.VMEM((NZ, NY, CUT, 128), BF16),
            pltpu.VMEM((NZ, NY, CUT, 128), BF16),
            pltpu.VMEM((len(STRADDLERS), CUT, 128), BF16),
            pltpu.VMEM((2, CUT, 128), BF16),
            pltpu.VMEM((2, CUT, 128), BF16),
            pltpu.VMEM((2, CUT, CUT, 128), BF16),
            pltpu.VMEM((2, CUT, CUT, 128), BF16),
            pltpu.VMEM((2, CUT, CUT, 128), BF16),
            pltpu.VMEM((32, 128), F32),
            pltpu.VMEM((CUT, 128), F32),
            pltpu.VMEM((128, 128), F32),
            pltpu.VMEM((256, 128), F32),
            pltpu.VMEM((1, 128), F32),
            pltpu.VMEM((1, 128), F32),
            pltpu.VMEM((2, 128), jnp.int32),
            pltpu.SMEM((2, 128), jnp.int32),
            pltpu.SMEM((2, 128), jnp.int32),
            pltpu.SMEM((1, 128), F32),
            pltpu.SMEM((1, 128), F32),
            dma((32,)), dma((32,)), dma((2,)), dma((32,)), dma((8,)), dma((8,)),
            dma((32,)), dma((32,)), dma((32,)), dma((2,)), dma((3,)), dma((3,)), dma((5,)),
        ],
        compiler_params=pltpu.CompilerParams(
            collective_id=0, has_side_effects=True, vmem_limit_bytes=48 * 2**20
        ),
    )(
        pair_models, blocks, weights, coverage, offsets[0].T, counts, psf_y, resample_y, psf_x, resample_x
    )
    return updated.reshape(BANDS, 32, 2, 128).transpose(2, 0, 1, 3).reshape(1, 2, BANDS, PIX2)


def solution(mesh):
    return jax.shard_map(
        on_device,
        mesh=mesh,
        in_specs=(
            P("blend", "epoch", None, None),
            P("epoch", "blend", None),
            P("epoch", "blend"),
            P("epoch", "blend"),
            P("epoch", "blend", None),
            P("blend", "epoch"),
            P("epoch", None),
            P("epoch", None),
            P("epoch", None),
            P("epoch", None),
        ),
        out_specs=P("blend", "epoch", None, None),
        check_vma=False,
    )
```

```python
import functools

import jax
import jax.numpy as jnp
from jax import lax
from jax.experimental import pallas as pl
from jax.experimental.pallas import tpu as pltpu
from jax.sharding import PartitionSpec as P

CUT = 64
BANDS = 6
PIX2 = 4096
E = 64
NY, NZ = 4, 8
step_size = 0.5
MESH = pl.DeviceIdType.MESH
F32, BF16 = jnp.float32, jnp.bfloat16


def band_of(epoch):
    return epoch * BANDS // E


STRADDLERS = [
    (y, z) for y in range(NY) for z in range(NZ) if band_of((y * NZ + z) * 2) != band_of((y * NZ + z) * 2 + 1)
]


def kernel(
    models_h, obs_hbm, weights_h, coverage_h, offs_h, counts_h, psf_y_h, res_y_h, psf_x_h, res_x_h, out,
    models, weights, coverage, offs, counts, psf_y, res_y, psf_x, res_x, obs_v, obs_st, obs_in, models_low, mod_in, term_out, term_out2, term_in, term_in2,
    mats, mats_in, tab_a, tab_at, tab_r, fold, rows_f, wide, spread,
    scale_v, scale_in, offs_in, off_own, off_par, sc_own, sc_par,
    in_s, in_r, in2_s, in2_r, obs_s, obs_r, t_s, t_r, t2_s, t2_r, small_s, small_r, local,
):
    me = lax.axis_index("epoch")
    x = lax.rem(me, 2)
    z = lax.rem(lax.div(me, 2), NZ)
    y = lax.div(me, 2 * NZ)
    partner = me + 1 - 2 * x

    def device(yy, zz):
        return (yy * NZ + zz) * 2 + x

    def place(ky, kz):
        return lax.rem(y + ky, NY), lax.rem(z + kz, NZ)

    relative = [(ky, kz) for kz in (4, 3, 5, 2, 6, 1, 7, 0) for ky in (2, 1, 3, 0)]
    others = [r for r in relative if r != (0, 0)]

    def remote(src, dst, send, recv, target):
        return pltpu.make_async_remote_copy(
            src_ref=src, dst_ref=dst, send_sem=send, recv_sem=recv, device_id={"epoch": target}, device_id_type=MESH
        )

    barrier = pltpu.get_barrier_semaphore()
    pl.semaphore_signal(barrier, inc=1, device_id={"epoch": partner}, device_id_type=MESH)
    for ky, kz in others:
        pl.semaphore_signal(barrier, inc=1, device_id={"epoch": device(*place(ky, kz))}, device_id_type=MESH)

    mat_loads = [
        pltpu.make_async_copy(src, dst, local.at[6 + i])
        for i, (src, dst) in enumerate(((psf_y_h, psf_y), (res_y_h, res_y), (psf_x_h, psf_x), (res_x_h, res_x)))
    ]
    load_models = pltpu.make_async_copy(models_h, models, local.at[5])
    load_obs = pltpu.make_async_copy(obs_hbm, obs_v, local.at[0])
    load_off = pltpu.make_async_copy(offs_h, off_own, local.at[1])
    small_loads = [
        pltpu.make_async_copy(src, dst, local.at[10 + i])
        for i, (src, dst) in enumerate(
            ((weights_h, weights), (coverage_h, coverage), (offs_h, offs), (counts_h, counts))
        )
    ]
    for load in mat_loads + [load_models, load_obs, load_off] + small_loads:
        load.start()

    straddle = jnp.int32(0)
    straddle_id = jnp.int32(0)
    for i, (ys, zs) in enumerate(STRADDLERS):
        hit = jnp.where(jnp.logical_and(y == ys, z == zs), 1, 0).astype(jnp.int32)
        straddle = straddle + hit
        straddle_id = straddle_id + i * hit

    lane = lax.broadcasted_iota(jnp.int32, (CUT, 128), 1)
    row = lax.broadcasted_iota(jnp.int32, (CUT, 128), 0)
    low = lane < CUT
    low_half = low[:32]
    even = lax.rem(row, 2) == 0
    mask_lo = jnp.where(low, 1.0, 0.0).astype(BF16)
    mask_hi = jnp.where(low, 0.0, 1.0).astype(BF16)

    def swap(v):
        turned = pltpu.roll(v, CUT, 1)
        up = pltpu.roll(turned, CUT - 1, 0)
        down = pltpu.roll(turned, 1, 0)
        return jnp.where(low, jnp.where(even, v, down), jnp.where(even, up, v))

    def unfold(ref):
        v = ref[...].astype(F32)
        for k in range(32):
            fold[k : k + 1, :] = v[:, k * 128 : (k + 1) * 128]
        top = fold[...]
        return top, pltpu.roll(top, CUT, 1)

    def natural(ref):
        top, bottom = unfold(ref)
        rows_f[pl.ds(0, 32, stride=2), :] = top
        rows_f[pl.ds(1, 32, stride=2), :] = bottom
        return rows_f[...]

    def doubled(v):
        return jnp.where(low, v, pltpu.roll(v, CUT, 1))

    for load in mat_loads:
        load.wait()
    top, bottom = unfold(psf_y)
    first = jnp.concatenate([top, bottom], axis=0)[:, :CUT].astype(BF16)
    second = doubled(natural(res_y)).astype(BF16)
    mats[0] = jnp.dot(first, second, preferred_element_type=F32).astype(BF16)
    first = natural(psf_x)[:, :CUT].astype(BF16)
    second = doubled(natural(res_x)).astype(BF16)
    mats[1] = jnp.dot(first, second, preferred_element_type=F32).astype(BF16)

    load_models.wait()
    for c in range(BANDS):
        models_low[c] = swap(models[c]).astype(BF16)

    def tables(slot, source):
        left = source[0].astype(F32)
        right = source[1].astype(F32)
        wide[...] = jnp.concatenate([left, left], axis=0).T

        def one(d, carry):
            tab_a[slot, d] = pltpu.roll(left, d, 1).astype(BF16)
            tab_at[slot, d] = wide[pl.ds(CUT - d, CUT), :].astype(BF16)
            tab_r[slot, d] = pltpu.roll(right, d, 1).astype(BF16)
            return carry

        lax.fori_loop(0, CUT, one, 0, unroll=4)

    load_obs.wait()

    def relayout(m, carry):
        spread[...] = obs_v[m].astype(F32)
        yy = lax.div(m, 4)
        z2 = 2 * lax.rem(m, 4)
        for s in range(4):
            f0 = spread[pl.ds(2 * s, 32, stride=8), :]
            f1 = spread[pl.ds(2 * s + 1, 32, stride=8), :]
            top = jnp.where(low_half, f0, pltpu.roll(f1, CUT, 1))
            bottom = jnp.where(low_half, pltpu.roll(f0, CUT, 1), f1)
            obs_st[s % 2, z2 + s // 2, yy] = jnp.concatenate([top, bottom], axis=0).astype(BF16)
        return carry

    lax.fori_loop(0, 16, relayout, 0)

    load_off.wait()
    for load in small_loads:
        load.wait()
    scale_v[...] = weights[...] * coverage[...].astype(F32)
    load_scale = pltpu.make_async_copy(scale_v, sc_own, local.at[2])
    load_scale.start()
    load_scale.wait()

    pl.semaphore_wait(barrier, 32)

    send_mats = remote(mats, mats_in, small_s.at[0], small_r.at[0], partner)
    send_off = remote(offs, offs_in, small_s.at[1], small_r.at[1], partner)
    send_scale = remote(scale_v, scale_in, small_s.at[2], small_r.at[2], partner)
    send_mats.start()
    send_off.start()
    send_scale.start()

    def obs_copy(g):
        zz = lax.rem(z + far_first(g), NZ)
        return remote(obs_st.at[1 - x, zz], obs_in.at[zz], obs_s.at[g], obs_r.at[g], partner)

    def far_first(g):
        return 4 + lax.div(g + 1, 2) * (1 - 2 * lax.rem(g, 2))

    for g in range(8):
        obs_copy(jnp.int32(g)).start()

    def model_copy(ky, kz):
        yy, zz = place(ky, kz)
        band = lax.div((yy * NZ + zz) * 2 * BANDS, E)
        return remote(
            models_low.at[band], mod_in.at[0, z, y], in_s.at[zz * NY + yy], in_r.at[z * NY + y], device(yy, zz)
        )

    for ky, kz in others:
        model_copy(ky, kz).start()
    for i, (ys, zs) in enumerate(STRADDLERS):
        band = band_of((ys * NZ + zs) * 2 + 1)
        here = jnp.logical_and(y == ys, z == zs)

        @pl.when(jnp.logical_not(here))
        def _():
            remote(
                models_low.at[band], mod_in.at[1, z, y], in2_s.at[i], in2_r.at[z * NY + y], device(ys, zs)
            ).start()

        @pl.when(here)
        def _():
            mod_in[1, z, y] = models_low[band]

    mod_in[0, z, y] = models_low[lax.div((y * NZ + z) * 2 * BANDS, E)]

    tables(0, mats)
    send_mats.wait_recv()
    tables(1, mats_in)
    send_off.wait_recv()
    send_scale.wait_recv()
    load_off = pltpu.make_async_copy(offs_in, off_par, local.at[3])
    load_scale = pltpu.make_async_copy(scale_in, sc_par, local.at[4])
    load_off.start()
    load_scale.start()
    load_off.wait()
    load_scale.wait()

    slot_own = straddle * x
    slot_par = straddle * (1 - x)
    own_first = slot_own == 0
    par_first = slot_par == 0
    offsets = (off_own, off_par)
    scales = (sc_own, sc_par)

    def term_copy(yy, zz):
        return remote(
            term_out.at[zz, yy], term_in.at[z, y], t_s.at[zz * NY + yy], t_r.at[z * NY + y], device(yy, zz)
        )

    def term2_copy(yy, zz):
        return remote(
            term_out2.at[zz, yy], term_in2.at[straddle_id], t2_s.at[zz * NY + yy], t2_r.at[straddle_id], device(yy, zz)
        )

    def split(v):
        return jnp.concatenate([v * mask_lo, v * mask_hi], axis=0)

    def group(g, carry):
        zz = lax.rem(z + far_first(g), NZ)
        obs_copy(g).wait_recv()
        units = []
        for ky in (2, 1, 3, 0):
            yy = lax.rem(y + ky, NY)

            def arrive():
                slot = zz * NY + yy
                remote(models_low.at[0], mod_in.at[0, zz, yy], in_s.at[slot], in_r.at[slot], partner).wait_recv()

                @pl.when(straddle == 1)
                def _():
                    remote(models_low.at[0], mod_in.at[1, zz, yy], in_s.at[slot], in2_r.at[slot], partner).wait_recv()

            if ky == 0:
                pl.when(g < 7)(arrive)
            else:
                arrive()
            for e in range(2):
                units.append((yy, e))
        state = []
        for yy, e in units:
            b = 2 * ((yy * NZ + zz) * 2 + x)
            dy0, dx0 = offsets[e][0, b], offsets[e][1, b]
            dy1, dx1 = offsets[e][0, b + 1], offsets[e][1, b + 1]
            left = tab_a[e, dy0] * mask_lo + tab_a[e, dy1] * mask_hi
            image = mod_in[slot_own if e == 0 else slot_par, zz, yy]
            blurred = jnp.dot(left, split(image), preferred_element_type=F32).astype(BF16)
            state.append([yy, e, b, dy0, dy1, dx0, dx1, blurred])
        for s in state:
            yy, e, b, dy0, dy1, dx0, dx1, blurred = s
            right = jnp.concatenate([tab_r[e, dx0] * mask_lo, tab_r[e, dx1] * mask_hi], axis=0)
            predicted = lax.dot_general(blurred, right, (((1,), (1,)), ((), ())), preferred_element_type=F32)
            seen = (obs_st[x, zz, yy] if e == 0 else obs_in[zz, yy]).astype(F32)
            scale = jnp.where(low[:1], scales[e][0, b], scales[e][0, b + 1])
            s.append((scale * (predicted - seen)).astype(BF16))
        for s in state:
            yy, e, b, dy0, dy1, dx0, dx1, blurred, misfit = s
            left_t = tab_at[e, dy0] * mask_lo + tab_at[e, dy1] * mask_hi
            s.append(jnp.dot(left_t, split(misfit), preferred_element_type=F32).astype(BF16))
        terms = {}
        for s in state:
            yy, e, b, dy0, dy1, dx0, dx1, blurred, misfit, back = s
            right = jnp.concatenate([tab_r[e, dx0] * mask_lo, tab_r[e, dx1] * mask_hi], axis=0)
            terms.setdefault(len(terms) if e == 0 else len(terms) - 1, [yy]).append(
                jnp.dot(back, right, preferred_element_type=F32)
            )
        for yy, own, par in terms.values():
            zero = jnp.zeros_like(own)
            term_out[zz, yy] = (jnp.where(own_first, own, zero) + jnp.where(par_first, par, zero)).astype(BF16)
            term_out2[zz, yy] = (jnp.where(own_first, zero, own) + jnp.where(par_first, zero, par)).astype(BF16)
        for ky in (2, 1, 3, 0):
            yy = lax.rem(y + ky, NY)

            def ship():
                term_copy(yy, zz).start()

                @pl.when(straddle == 1)
                def _():
                    term2_copy(yy, zz).start()

            if ky == 0:
                pl.when(g < 7)(ship)
            else:
                ship()
        return carry

    lax.fori_loop(0, 8, group, 0)

    term_in[z, y] = term_out[z, y]

    @pl.when(straddle == 1)
    def _():
        term_in2[straddle_id] = term_out2[z, y]

    for ky, kz in others:
        yy, zz = place(ky, kz)
        slot = zz * NY + yy
        remote(term_out.at[zz, yy], term_in.at[zz, yy], t_s.at[slot], t_r.at[slot], partner).wait_recv()
    for i, (ys, zs) in enumerate(STRADDLERS):

        @pl.when(jnp.logical_not(jnp.logical_and(y == ys, z == zs)))
        def _():
            remote(term_out2.at[0, 0], term_in2.at[i], t2_s.at[0], t2_r.at[i], partner).wait_recv()

    seen_by = jnp.where(even, counts[0, 0].astype(F32), counts[0, 1].astype(F32))
    factor = step_size / seen_by
    for c in range(BANDS):
        total = jnp.zeros((CUT, 128), F32)
        for yy in range(NY):
            for zz in range(NZ):
                if band_of((yy * NZ + zz) * 2) == c:
                    total = total + term_in[zz, yy].astype(F32)
        for i, (ys, zs) in enumerate(STRADDLERS):
            if band_of((ys * NZ + zs) * 2 + 1) == c:
                total = total + term_in2[i].astype(F32)
        out[c] = models[c] - factor * swap(total)

    send_mats.wait_send()
    send_off.wait_send()
    send_scale.wait_send()
    for g in range(8):
        obs_copy(jnp.int32(g)).wait_send()
    for ky, kz in others:
        model_copy(ky, kz).wait_send()
        yy, zz = place(ky, kz)
        term_copy(yy, zz).wait_send()

        @pl.when(straddle == 1)
        def _():
            term2_copy(yy, zz).wait_send()

    for i, (ys, zs) in enumerate(STRADDLERS):

        @pl.when(jnp.logical_not(jnp.logical_and(y == ys, z == zs)))
        def _():
            remote(models_low.at[0], mod_in.at[1, z, y], in2_s.at[i], in2_r.at[0], partner).wait_send()


def on_device(
    models, observed, weights, coverage, offsets, counts, psf_y, resample_y, psf_x, resample_x
):
    pair_models = models[0].reshape(2, BANDS, 32, 128).transpose(1, 2, 0, 3).reshape(BANDS, CUT, 128)
    blocks = observed[0].reshape(16, 8, 32, 128).transpose(0, 2, 1, 3).reshape(16, 256, 128)
    vmem = pl.BlockSpec(memory_space=pltpu.VMEM)
    dma = pltpu.SemaphoreType.DMA
    updated = pl.pallas_call(
        kernel,
        out_shape=jax.ShapeDtypeStruct((BANDS, CUT, 128), F32),
        in_specs=[pl.BlockSpec(memory_space=pltpu.HBM)] * 10,
        out_specs=vmem,
        scratch_shapes=[
            pltpu.VMEM((BANDS, CUT, 128), F32),
            pltpu.VMEM((1, 128), F32),
            pltpu.VMEM((1, 128), jnp.int32),
            pltpu.VMEM((2, 128), jnp.int32),
            pltpu.SMEM((1, 2), jnp.int32),
            pltpu.VMEM((1, PIX2), BF16),
            pltpu.VMEM((1, PIX2), BF16),
            pltpu.VMEM((1, PIX2), BF16),
            pltpu.VMEM((1, PIX2), BF16),
            pltpu.VMEM((16, 256, 128), BF16),
            pltpu.VMEM((2, NZ, NY, CUT, 128), BF16),
            pltpu.VMEM((NZ, NY, CUT, 128), BF16),
            pltpu.VMEM((BANDS, CUT, 128), BF16),
            pltpu.VMEM((2, NZ, NY, CUT, 128), BF16),
            pltpu.VMEM((NZ, NY, CUT, 128), BF16),
            pltpu.VMEM((NZ, NY, CUT, 128), BF16),
            pltpu.VMEM((NZ, NY, CUT, 128), BF16),
            pltpu.VMEM((len(STRADDLERS), CUT, 128), BF16),
            pltpu.VMEM((2, CUT, 128), BF16),
            pltpu.VMEM((2, CUT, 128), BF16),
            pltpu.VMEM((2, CUT, CUT, 128), BF16),
            pltpu.VMEM((2, CUT, CUT, 128), BF16),
            pltpu.VMEM((2, CUT, CUT, 128), BF16),
            pltpu.VMEM((32, 128), F32),
            pltpu.VMEM((CUT, 128), F32),
            pltpu.VMEM((128, 128), F32),
            pltpu.VMEM((256, 128), F32),
            pltpu.VMEM((1, 128), F32),
            pltpu.VMEM((1, 128), F32),
            pltpu.VMEM((2, 128), jnp.int32),
            pltpu.SMEM((2, 128), jnp.int32),
            pltpu.SMEM((2, 128), jnp.int32),
            pltpu.SMEM((1, 128), F32),
            pltpu.SMEM((1, 128), F32),
            dma((32,)), dma((32,)), dma((2,)), dma((32,)), dma((8,)), dma((8,)),
            dma((32,)), dma((32,)), dma((32,)), dma((2,)), dma((3,)), dma((3,)), dma((14,)),
        ],
        compiler_params=pltpu.CompilerParams(
            collective_id=0, has_side_effects=True, vmem_limit_bytes=67043328
        ),
    )(
        pair_models, blocks, weights, coverage, offsets[0].T, counts, psf_y, resample_y, psf_x, resample_x
    )
    return updated.reshape(BANDS, 32, 2, 128).transpose(2, 0, 1, 3).reshape(1, 2, BANDS, PIX2)


def solution(mesh):
    return jax.shard_map(
        on_device,
        mesh=mesh,
        in_specs=(
            P("blend", "epoch", None, None),
            P("epoch", "blend", None),
            P("epoch", "blend"),
            P("epoch", "blend"),
            P("epoch", "blend", None),
            P("blend", "epoch"),
            P("epoch", None),
            P("epoch", None),
            P("epoch", None),
            P("epoch", None),
        ),
        out_specs=P("blend", "epoch", None, None),
        check_vma=False,
    )
```

```python
import functools

import jax
import jax.numpy as jnp
from jax import lax
from jax.experimental import pallas as pl
from jax.experimental.pallas import tpu as pltpu
from jax.sharding import PartitionSpec as P

CUT = 64
BANDS = 6
PIX2 = 4096
E = 64
NY, NZ = 4, 8
step_size = 0.5
MESH = pl.DeviceIdType.MESH
F32, BF16 = jnp.float32, jnp.bfloat16


def band_of(epoch):
    return epoch * BANDS // E


STRADDLERS = [
    (y, z) for y in range(NY) for z in range(NZ) if band_of((y * NZ + z) * 2) != band_of((y * NZ + z) * 2 + 1)
]


def kernel(
    models_h, obs_hbm, weights_h, coverage_h, offs_h, counts_h, psf_y_h, res_y_h, psf_x_h, res_x_h, out_h,
    out, models, weights, coverage, offs, counts, psf_y, res_y, psf_x, res_x, obs_v, obs_st, obs_in, models_low, mod_in, term_out, term_out2, term_in, term_in2,
    mats, mats_in, tab_a, tab_at, tab_r, fold, rows_f, wide, spread,
    scale_v, scale_in, offs_in, off_own, off_par, sc_own, sc_par,
    in_s, in_r, in2_s, in2_r, obs_s, obs_r, t_s, t_r, t2_s, t2_r, small_s, small_r, local, out_sem,
):
    me = lax.axis_index("epoch")
    x = lax.rem(me, 2)
    z = lax.rem(lax.div(me, 2), NZ)
    y = lax.div(me, 2 * NZ)
    partner = me + 1 - 2 * x

    def device(yy, zz):
        return (yy * NZ + zz) * 2 + x

    def place(ky, kz):
        return lax.rem(y + ky, NY), lax.rem(z + kz, NZ)

    relative = [(ky, kz) for kz in (4, 3, 5, 2, 6, 1, 7, 0) for ky in (2, 1, 3, 0)]
    others = [r for r in relative if r != (0, 0)]

    def remote(src, dst, send, recv, target):
        return pltpu.make_async_remote_copy(
            src_ref=src, dst_ref=dst, send_sem=send, recv_sem=recv, device_id={"epoch": target}, device_id_type=MESH
        )

    barrier = pltpu.get_barrier_semaphore()
    pl.semaphore_signal(barrier, inc=1, device_id={"epoch": partner}, device_id_type=MESH)
    for ky, kz in others:
        pl.semaphore_signal(barrier, inc=1, device_id={"epoch": device(*place(ky, kz))}, device_id_type=MESH)

    mat_loads = [
        pltpu.make_async_copy(src, dst, local.at[6 + i])
        for i, (src, dst) in enumerate(((psf_y_h, psf_y), (res_y_h, res_y), (psf_x_h, psf_x), (res_x_h, res_x)))
    ]
    load_models = pltpu.make_async_copy(models_h, models, local.at[5])
    load_obs = pltpu.make_async_copy(obs_hbm, obs_v, local.at[0])
    load_off = pltpu.make_async_copy(offs_h, off_own, local.at[1])
    small_loads = [
        pltpu.make_async_copy(src, dst, local.at[10 + i])
        for i, (src, dst) in enumerate(
            ((weights_h, weights), (coverage_h, coverage), (offs_h, offs), (counts_h, counts))
        )
    ]
    for load in mat_loads + [load_models, load_obs, load_off] + small_loads:
        load.start()

    straddle = jnp.int32(0)
    straddle_id = jnp.int32(0)
    for i, (ys, zs) in enumerate(STRADDLERS):
        hit = jnp.where(jnp.logical_and(y == ys, z == zs), 1, 0).astype(jnp.int32)
        straddle = straddle + hit
        straddle_id = straddle_id + i * hit

    lane = lax.broadcasted_iota(jnp.int32, (CUT, 128), 1)
    row = lax.broadcasted_iota(jnp.int32, (CUT, 128), 0)
    low = lane < CUT
    low_half = low[:32]
    even = lax.rem(row, 2) == 0
    mask_lo = jnp.where(low, 1.0, 0.0).astype(BF16)
    mask_hi = jnp.where(low, 0.0, 1.0).astype(BF16)

    def swap(v):
        turned = pltpu.roll(v, CUT, 1)
        up = pltpu.roll(turned, CUT - 1, 0)
        down = pltpu.roll(turned, 1, 0)
        return jnp.where(low, jnp.where(even, v, down), jnp.where(even, up, v))

    def unfold(ref):
        v = ref[...].astype(F32)
        for k in range(32):
            fold[k : k + 1, :] = v[:, k * 128 : (k + 1) * 128]
        top = fold[...]
        return top, pltpu.roll(top, CUT, 1)

    def natural(ref):
        top, bottom = unfold(ref)
        rows_f[pl.ds(0, 32, stride=2), :] = top
        rows_f[pl.ds(1, 32, stride=2), :] = bottom
        return rows_f[...]

    def doubled(v):
        return jnp.where(low, v, pltpu.roll(v, CUT, 1))

    load_models.wait()
    for c in range(BANDS):
        models_low[c] = swap(models[c]).astype(BF16)

    def tables(slot, source):
        left = source[0].astype(F32)
        right = source[1].astype(F32)
        wide[...] = jnp.concatenate([left, left], axis=0).T

        def one(d, carry):
            tab_a[slot, d] = pltpu.roll(left, d, 1).astype(BF16)
            tab_at[slot, d] = wide[pl.ds(CUT - d, CUT), :].astype(BF16)
            tab_r[slot, d] = pltpu.roll(right, d, 1).astype(BF16)
            return carry

        lax.fori_loop(0, CUT, one, 0, unroll=4)

    pl.semaphore_wait(barrier, 32)

    def far_first(g):
        return 4 + lax.div(g + 1, 2) * (1 - 2 * lax.rem(g, 2))

    def model_copy(ky, kz):
        yy, zz = place(ky, kz)
        band = lax.div((yy * NZ + zz) * 2 * BANDS, E)
        return remote(
            models_low.at[band], mod_in.at[0, z * NY + y], in_s, in_r.at[z], device(yy, zz)
        )

    for ky, kz in others:
        model_copy(ky, kz).start()
    for i, (ys, zs) in enumerate(STRADDLERS):
        band = band_of((ys * NZ + zs) * 2 + 1)
        here = jnp.logical_and(y == ys, z == zs)

        @pl.when(jnp.logical_not(here))
        def _():
            remote(
                models_low.at[band], mod_in.at[1, z * NY + y], in2_s.at[i], in2_r.at[z], device(ys, zs)
            ).start()

        @pl.when(here)
        def _():
            mod_in[1, z * NY + y] = models_low[band]

    mod_in[0, z * NY + y] = models_low[lax.div((y * NZ + z) * 2 * BANDS, E)]

    for load in mat_loads:
        load.wait()
    top, bottom = unfold(psf_y)
    first = jnp.concatenate([top, bottom], axis=0)[:, :CUT].astype(BF16)
    second = doubled(natural(res_y)).astype(BF16)
    mats[0] = jnp.dot(first, second, preferred_element_type=F32).astype(BF16)
    first = natural(psf_x)[:, :CUT].astype(BF16)
    second = doubled(natural(res_x)).astype(BF16)
    mats[1] = jnp.dot(first, second, preferred_element_type=F32).astype(BF16)

    for load in small_loads:
        load.wait()
    scale_v[...] = weights[...] * coverage[...].astype(F32)
    send_mats = remote(mats, mats_in, small_s.at[0], small_r.at[0], partner)
    send_off = remote(offs, offs_in, small_s.at[1], small_r.at[1], partner)
    send_scale = remote(scale_v, scale_in, small_s.at[2], small_r.at[2], partner)
    send_mats.start()
    send_off.start()
    send_scale.start()
    load_scale = pltpu.make_async_copy(scale_v, sc_own, local.at[2])
    load_scale.start()

    load_obs.wait()

    def relayout(z2):
        def rows(yy, carry):
            spread[...] = obs_v[yy * 4 + z2].astype(F32)
            for s in range(4):
                f0 = spread[pl.ds(2 * s, 32, stride=8), :]
                f1 = spread[pl.ds(2 * s + 1, 32, stride=8), :]
                top = jnp.where(low_half, f0, pltpu.roll(f1, CUT, 1))
                bottom = jnp.where(low_half, pltpu.roll(f0, CUT, 1), f1)
                obs_st[s % 2, 2 * z2 + s // 2, yy] = jnp.concatenate([top, bottom], axis=0).astype(BF16)
            return carry

        lax.fori_loop(0, NY, rows, 0)

    def obs_copy(g):
        zz = lax.rem(z + far_first(g), NZ)
        return remote(obs_st.at[1 - x, zz], obs_in.at[zz], obs_s, obs_r.at[g], partner)

    farthest = lax.div(lax.rem(z + 4, NZ), 2)
    for steps, groups in (((0,), (0,)), ((3, 1), (1, 2, 3, 4)), ((2,), (5, 6, 7))):
        for step in steps:
            relayout(lax.rem(farthest + step, 4))
        for g in groups:
            obs_copy(jnp.int32(g)).start()

    tables(0, mats)
    send_mats.wait_recv()
    tables(1, mats_in)
    send_off.wait_recv()
    send_scale.wait_recv()
    load_off.wait()
    load_scale.wait()
    load_off = pltpu.make_async_copy(offs_in, off_par, local.at[3])
    load_scale = pltpu.make_async_copy(scale_in, sc_par, local.at[4])
    load_off.start()
    load_scale.start()
    load_off.wait()
    load_scale.wait()

    slot_own = straddle * x
    slot_par = straddle * (1 - x)
    own_first = slot_own == 0
    par_first = slot_par == 0
    offsets = (off_own, off_par)
    scales = (sc_own, sc_par)

    def term_copy(yy, zz):
        return remote(
            term_out.at[zz * NY + yy], term_in.at[z * NY + y], t_s, t_r, device(yy, zz)
        )

    def term2_copy(yy, zz):
        return remote(
            term_out2.at[zz * NY + yy], term_in2.at[straddle_id], t2_s, t2_r.at[straddle_id], device(yy, zz)
        )

    def arrived(tiles, semaphore):
        pltpu.make_async_copy(tiles, tiles, semaphore).wait()

    def split(v):
        return jnp.concatenate([v * mask_lo, v * mask_hi], axis=0)

    def group(g, carry):
        zz = lax.rem(z + far_first(g), NZ)
        obs_copy(g).wait_recv()

        def arrive(count):
            tiles = pl.ds(zz * NY, count)
            arrived(mod_in.at[0, tiles], in_r.at[zz])

            @pl.when(straddle == 1)
            def _():
                arrived(mod_in.at[1, tiles], in2_r.at[zz])

        pl.when(g < 7)(lambda: arrive(NY))
        pl.when(g == 7)(lambda: arrive(NY - 1))
        units = []
        for ky in (2, 1, 3, 0):
            yy = lax.rem(y + ky, NY)
            for e in range(2):
                units.append((yy, e))
        state = []
        for yy, e in units:
            b = 2 * ((yy * NZ + zz) * 2 + x)
            dy0, dx0 = offsets[e][0, b], offsets[e][1, b]
            dy1, dx1 = offsets[e][0, b + 1], offsets[e][1, b + 1]
            left = tab_a[e, dy0] * mask_lo + tab_a[e, dy1] * mask_hi
            image = mod_in[slot_own if e == 0 else slot_par, zz * NY + yy]
            blurred = jnp.dot(left, split(image), preferred_element_type=F32).astype(BF16)
            state.append([yy, e, b, dy0, dy1, dx0, dx1, blurred])
        for s in state:
            yy, e, b, dy0, dy1, dx0, dx1, blurred = s
            right = jnp.concatenate([tab_r[e, dx0] * mask_lo, tab_r[e, dx1] * mask_hi], axis=0)
            predicted = lax.dot_general(blurred, right, (((1,), (1,)), ((), ())), preferred_element_type=F32)
            seen = (obs_st[x, zz, yy] if e == 0 else obs_in[zz, yy]).astype(F32)
            scale = jnp.where(low[:1], scales[e][0, b], scales[e][0, b + 1])
            s.append((scale * (predicted - seen)).astype(BF16))
        for s in state:
            yy, e, b, dy0, dy1, dx0, dx1, blurred, misfit = s
            left_t = tab_at[e, dy0] * mask_lo + tab_at[e, dy1] * mask_hi
            s.append(jnp.dot(left_t, split(misfit), preferred_element_type=F32).astype(BF16))
        terms = {}
        for s in state:
            yy, e, b, dy0, dy1, dx0, dx1, blurred, misfit, back = s
            right = jnp.concatenate([tab_r[e, dx0] * mask_lo, tab_r[e, dx1] * mask_hi], axis=0)
            terms.setdefault(len(terms) if e == 0 else len(terms) - 1, [yy]).append(
                jnp.dot(back, right, preferred_element_type=F32)
            )
        for yy, own, par in terms.values():
            zero = jnp.zeros_like(own)
            term_out[zz * NY + yy] = (jnp.where(own_first, own, zero) + jnp.where(par_first, par, zero)).astype(BF16)
            term_out2[zz * NY + yy] = (jnp.where(own_first, zero, own) + jnp.where(par_first, zero, par)).astype(BF16)
        for ky in (2, 1, 3, 0):
            yy = lax.rem(y + ky, NY)

            def ship():
                term_copy(yy, zz).start()

                @pl.when(straddle == 1)
                def _():
                    term2_copy(yy, zz).start()

            if ky == 0:
                pl.when(g < 7)(ship)
            else:
                ship()
        return carry

    lax.fori_loop(0, 8, group, 0)

    term_in[z * NY + y] = term_out[z * NY + y]

    @pl.when(straddle == 1)
    def _():
        term_in2[straddle_id] = term_out2[z * NY + y]

    send_mats.wait_send()
    send_off.wait_send()
    send_scale.wait_send()
    arrived(obs_in, obs_s)
    arrived(mod_in.at[0, pl.ds(0, 31)], in_s)
    for i, (ys, zs) in enumerate(STRADDLERS):

        @pl.when(jnp.logical_not(jnp.logical_and(y == ys, z == zs)))
        def _():
            arrived(models_low.at[0], in2_s.at[i])

    arrived(term_in.at[pl.ds(0, 31)], t_r)
    for i, (ys, zs) in enumerate(STRADDLERS):

        @pl.when(jnp.logical_not(jnp.logical_and(y == ys, z == zs)))
        def _():
            arrived(term_in2.at[i], t2_r.at[i])

    seen_by = jnp.where(even, counts[0, 0].astype(F32), counts[0, 1].astype(F32))
    factor = step_size / seen_by
    for c in range(BANDS):
        total = jnp.zeros((CUT, 128), F32)
        for yy in range(NY):
            for zz in range(NZ):
                if band_of((yy * NZ + zz) * 2) == c:
                    total = total + term_in[zz * NY + yy].astype(F32)
        for i, (ys, zs) in enumerate(STRADDLERS):
            if band_of((ys * NZ + zs) * 2 + 1) == c:
                total = total + term_in2[i].astype(F32)
        out[c] = factor * swap(total)
        pltpu.make_async_copy(out.at[c], out_h.at[c], out_sem).start()

    arrived(term_out.at[pl.ds(0, 31)], t_s)

    @pl.when(straddle == 1)
    def _():
        arrived(term_out2.at[pl.ds(0, 31)], t2_s)

    arrived(out, out_sem)


def on_device(
    models, observed, weights, coverage, offsets, counts, psf_y, resample_y, psf_x, resample_x
):
    pair_models = models[0].reshape(2, BANDS, 32, 128).transpose(1, 2, 0, 3).reshape(BANDS, CUT, 128)
    blocks = observed[0].reshape(16, 8, 32, 128).transpose(0, 2, 1, 3).reshape(16, 256, 128)
    dma = pltpu.SemaphoreType.DMA
    change = pl.pallas_call(
        kernel,
        out_shape=jax.ShapeDtypeStruct((BANDS, CUT, 128), F32),
        in_specs=[pl.BlockSpec(memory_space=pltpu.HBM)] * 10,
        out_specs=pl.BlockSpec(memory_space=pl.ANY),
        scratch_shapes=[
            pltpu.VMEM((BANDS, CUT, 128), F32),
            pltpu.VMEM((BANDS, CUT, 128), F32),
            pltpu.VMEM((1, 128), F32),
            pltpu.VMEM((1, 128), jnp.int32),
            pltpu.VMEM((2, 128), jnp.int32),
            pltpu.SMEM((1, 2), jnp.int32),
            pltpu.VMEM((1, PIX2), BF16),
            pltpu.VMEM((1, PIX2), BF16),
            pltpu.VMEM((1, PIX2), BF16),
            pltpu.VMEM((1, PIX2), BF16),
            pltpu.VMEM((16, 256, 128), BF16),
            pltpu.VMEM((2, NZ, NY, CUT, 128), BF16),
            pltpu.VMEM((NZ, NY, CUT, 128), BF16),
            pltpu.VMEM((BANDS, CUT, 128), BF16),
            pltpu.VMEM((2, NZ * NY, CUT, 128), BF16),
            pltpu.VMEM((NZ * NY, CUT, 128), BF16),
            pltpu.VMEM((NZ * NY, CUT, 128), BF16),
            pltpu.VMEM((NZ * NY, CUT, 128), BF16),
            pltpu.VMEM((len(STRADDLERS), CUT, 128), BF16),
            pltpu.VMEM((2, CUT, 128), BF16),
            pltpu.VMEM((2, CUT, 128), BF16),
            pltpu.VMEM((2, CUT, CUT, 128), BF16),
            pltpu.VMEM((2, CUT, CUT, 128), BF16),
            pltpu.VMEM((2, CUT, CUT, 128), BF16),
            pltpu.VMEM((32, 128), F32),
            pltpu.VMEM((CUT, 128), F32),
            pltpu.VMEM((128, 128), F32),
            pltpu.VMEM((256, 128), F32),
            pltpu.VMEM((1, 128), F32),
            pltpu.VMEM((1, 128), F32),
            pltpu.VMEM((2, 128), jnp.int32),
            pltpu.SMEM((2, 128), jnp.int32),
            pltpu.SMEM((2, 128), jnp.int32),
            pltpu.SMEM((1, 128), F32),
            pltpu.SMEM((1, 128), F32),
            dma, dma((NZ,)), dma((2,)), dma((NZ,)), dma, dma((NZ,)),
            dma, dma, dma, dma((2,)), dma((3,)), dma((3,)), dma((14,)), dma,
        ],
        compiler_params=pltpu.CompilerParams(
            collective_id=0, has_side_effects=True, vmem_limit_bytes=60_000_000
        ),
    )(
        pair_models, blocks, weights, coverage, offsets[0].T, counts, psf_y, resample_y, psf_x, resample_x
    )
    updated = pair_models - change
    return updated.reshape(BANDS, 32, 2, 128).transpose(2, 0, 1, 3).reshape(1, 2, BANDS, PIX2)


def solution(mesh):
    return jax.shard_map(
        on_device,
        mesh=mesh,
        in_specs=(
            P("blend", "epoch", None, None),
            P("epoch", "blend", None),
            P("epoch", "blend"),
            P("epoch", "blend"),
            P("epoch", "blend", None),
            P("blend", "epoch"),
            P("epoch", None),
            P("epoch", None),
            P("epoch", None),
            P("epoch", None),
        ),
        out_specs=P("blend", "epoch", None, None),
        check_vma=False,
    )
```

```python
import functools

import jax
import jax.numpy as jnp
from jax import lax
from jax.experimental import pallas as pl
from jax.experimental.pallas import tpu as pltpu
from jax.sharding import PartitionSpec as P

CUT = 64
BANDS = 6
PIX2 = 4096
E = 64
NY, NZ = 4, 8
step_size = 0.5
MESH = pl.DeviceIdType.MESH
F32, BF16 = jnp.float32, jnp.bfloat16


def band_of(epoch):
    return epoch * BANDS // E


STRADDLERS = [
    (y, z) for y in range(NY) for z in range(NZ) if band_of((y * NZ + z) * 2) != band_of((y * NZ + z) * 2 + 1)
]


def kernel(
    models_h, obs_hbm, weights_h, coverage_h, offs_h, counts_h, psf_y_h, res_y_h, psf_x_h, res_x_h, out_h,
    out, models, weights, coverage, offs, counts, psf_y, res_y, psf_x, res_x, obs_v, obs_st, obs_in, models_low, mod_in, term_out, term_out2, term_in, term_in2,
    mats, mats_in, tab_a, tab_at, tab_r, fold, rows_f, wide, spread,
    scale_v, scale_in, offs_in, off_own, off_par, sc_own, sc_par,
    in_s, in_r, in2_s, in2_r, obs_s, obs_r, t_s, t_r, t2_s, t2_r, small_s, small_r, local, out_sem,
):
    me = lax.axis_index("epoch")
    x = lax.rem(me, 2)
    z = lax.rem(lax.div(me, 2), NZ)
    y = lax.div(me, 2 * NZ)
    partner = me + 1 - 2 * x

    def device(yy, zz):
        return (yy * NZ + zz) * 2 + x

    def place(ky, kz):
        return lax.rem(y + ky, NY), lax.rem(z + kz, NZ)

    relative = [(ky, kz) for kz in (4, 3, 5, 2, 6, 1, 7, 0) for ky in (2, 3, 1, 0)]
    others = [r for r in relative if r != (0, 0)]

    def remote(src, dst, send, recv, target):
        return pltpu.make_async_remote_copy(
            src_ref=src, dst_ref=dst, send_sem=send, recv_sem=recv, device_id={"epoch": target}, device_id_type=MESH
        )

    barrier = pltpu.get_barrier_semaphore()
    pl.semaphore_signal(barrier, inc=1, device_id={"epoch": partner}, device_id_type=MESH)
    for ky, kz in others:
        pl.semaphore_signal(barrier, inc=1, device_id={"epoch": device(*place(ky, kz))}, device_id_type=MESH)

    mat_loads = [
        pltpu.make_async_copy(src, dst, local.at[6 + i])
        for i, (src, dst) in enumerate(((psf_y_h, psf_y), (res_y_h, res_y), (psf_x_h, psf_x), (res_x_h, res_x)))
    ]
    load_models = pltpu.make_async_copy(models_h, models, local.at[5])
    load_obs = pltpu.make_async_copy(obs_hbm, obs_v, local.at[0])
    load_off = pltpu.make_async_copy(offs_h, off_own, local.at[1])
    small_loads = [
        pltpu.make_async_copy(src, dst, local.at[10 + i])
        for i, (src, dst) in enumerate(
            ((weights_h, weights), (coverage_h, coverage), (offs_h, offs), (counts_h, counts))
        )
    ]
    load_models.start()
    for load in mat_loads + [load_off] + small_loads:
        load.start()

    straddle = jnp.int32(0)
    straddle_id = jnp.int32(0)
    for i, (ys, zs) in enumerate(STRADDLERS):
        hit = jnp.where(jnp.logical_and(y == ys, z == zs), 1, 0).astype(jnp.int32)
        straddle = straddle + hit
        straddle_id = straddle_id + i * hit

    lane = lax.broadcasted_iota(jnp.int32, (CUT, 128), 1)
    row = lax.broadcasted_iota(jnp.int32, (CUT, 128), 0)
    low = lane < CUT
    low_half = low[:32]
    even = lax.rem(row, 2) == 0
    mask_lo = jnp.where(low, 1.0, 0.0).astype(BF16)
    mask_hi = jnp.where(low, 0.0, 1.0).astype(BF16)

    def swap(v):
        turned = pltpu.roll(v, CUT, 1)
        up = pltpu.roll(turned, CUT - 1, 0)
        down = pltpu.roll(turned, 1, 0)
        return jnp.where(low, jnp.where(even, v, down), jnp.where(even, up, v))

    def unfold(ref):
        v = ref[...].astype(F32)
        for k in range(32):
            fold[k : k + 1, :] = v[:, k * 128 : (k + 1) * 128]
        top = fold[...]
        return top, pltpu.roll(top, CUT, 1)

    def natural(ref):
        top, bottom = unfold(ref)
        rows_f[pl.ds(0, 32, stride=2), :] = top
        rows_f[pl.ds(1, 32, stride=2), :] = bottom
        return rows_f[...]

    def doubled(v):
        return jnp.where(low, v, pltpu.roll(v, CUT, 1))

    load_models.wait()
    load_obs.start()
    for c in range(BANDS):
        models_low[c] = swap(models[c]).astype(BF16)

    def tables(slot, source):
        left = source[0].astype(F32)
        right = source[1].astype(F32)
        wide[...] = jnp.concatenate([left, left], axis=0).T

        def one(d, carry):
            tab_a[slot, d] = pltpu.roll(left, d, 1).astype(BF16)
            tab_at[slot, d] = wide[pl.ds(CUT - d, CUT), :].astype(BF16)
            tab_r[slot, d] = pltpu.roll(right, d, 1).astype(BF16)
            return carry

        lax.fori_loop(0, CUT, one, 0, unroll=4)

    pl.semaphore_wait(barrier, 32)

    def far_first(g):
        return 4 + lax.div(g + 1, 2) * (1 - 2 * lax.rem(g, 2))

    def model_copy(ky, kz):
        yy, zz = place(ky, kz)
        band = lax.div((yy * NZ + zz) * 2 * BANDS, E)
        return remote(
            models_low.at[band], mod_in.at[0, z * NY + y], in_s, in_r.at[z], device(yy, zz)
        )

    for i, (ys, zs) in enumerate(STRADDLERS):
        band = band_of((ys * NZ + zs) * 2 + 1)
        here = jnp.logical_and(y == ys, z == zs)

        @pl.when(jnp.logical_not(here))
        def _():
            remote(
                models_low.at[band], mod_in.at[1, z * NY + y], in2_s.at[i], in2_r.at[z], device(ys, zs)
            ).start()

        @pl.when(here)
        def _():
            mod_in[1, z * NY + y] = models_low[band]

    for ky, kz in others:
        model_copy(ky, kz).start()

    mod_in[0, z * NY + y] = models_low[lax.div((y * NZ + z) * 2 * BANDS, E)]

    for load in mat_loads:
        load.wait()
    top, bottom = unfold(psf_y)
    first = jnp.concatenate([top, bottom], axis=0)[:, :CUT].astype(BF16)
    second = doubled(natural(res_y)).astype(BF16)
    mats[0] = jnp.dot(first, second, preferred_element_type=F32).astype(BF16)
    first = natural(psf_x)[:, :CUT].astype(BF16)
    second = doubled(natural(res_x)).astype(BF16)
    mats[1] = jnp.dot(first, second, preferred_element_type=F32).astype(BF16)

    for load in small_loads:
        load.wait()
    scale_v[...] = weights[...] * coverage[...].astype(F32)
    send_mats = remote(mats, mats_in, small_s.at[0], small_r.at[0], partner)
    send_off = remote(offs, offs_in, small_s.at[1], small_r.at[1], partner)
    send_scale = remote(scale_v, scale_in, small_s.at[2], small_r.at[2], partner)
    send_mats.start()
    send_off.start()
    send_scale.start()
    load_scale = pltpu.make_async_copy(scale_v, sc_own, local.at[2])
    load_scale.start()

    load_obs.wait()

    def relayout(z2):
        def rows(yy, carry):
            spread[...] = obs_v[yy * 4 + z2].astype(F32)
            for s in range(4):
                f0 = spread[pl.ds(2 * s, 32, stride=8), :]
                f1 = spread[pl.ds(2 * s + 1, 32, stride=8), :]
                top = jnp.where(low_half, f0, pltpu.roll(f1, CUT, 1))
                bottom = jnp.where(low_half, pltpu.roll(f0, CUT, 1), f1)
                obs_st[s % 2, 2 * z2 + s // 2, yy] = jnp.concatenate([top, bottom], axis=0).astype(BF16)
            return carry

        lax.fori_loop(0, NY, rows, 0)

    def obs_copy(g):
        zz = lax.rem(z + far_first(g), NZ)
        return remote(obs_st.at[1 - x, zz], obs_in.at[zz], obs_s, obs_r.at[g], partner)

    farthest = lax.div(lax.rem(z + 4, NZ), 2)
    for steps, groups in (((0,), (0,)), ((3, 1), (1, 2, 3, 4)), ((2,), (5, 6, 7))):
        for step in steps:
            relayout(lax.rem(farthest + step, 4))
        for g in groups:
            obs_copy(jnp.int32(g)).start()

    tables(0, mats)
    send_mats.wait_recv()
    tables(1, mats_in)
    send_off.wait_recv()
    send_scale.wait_recv()
    load_off.wait()
    load_scale.wait()
    load_off = pltpu.make_async_copy(offs_in, off_par, local.at[3])
    load_scale = pltpu.make_async_copy(scale_in, sc_par, local.at[4])
    load_off.start()
    load_scale.start()
    load_off.wait()
    load_scale.wait()

    slot_own = straddle * x
    slot_par = straddle * (1 - x)
    own_first = slot_own == 0
    par_first = slot_par == 0
    offsets = (off_own, off_par)
    scales = (sc_own, sc_par)

    def term_copy(yy, zz):
        return remote(
            term_out.at[zz * NY + yy], term_in.at[z * NY + y], t_s, t_r, device(yy, zz)
        )

    def term2_copy(yy, zz):
        return remote(
            term_out2.at[zz * NY + yy], term_in2.at[straddle_id], t2_s, t2_r.at[straddle_id], device(yy, zz)
        )

    def arrived(tiles, semaphore):
        pltpu.make_async_copy(tiles, tiles, semaphore).wait()

    def split(v):
        return jnp.concatenate([v * mask_lo, v * mask_hi], axis=0)

    def group(g, carry):
        zz = lax.rem(z + far_first(g), NZ)
        obs_copy(g).wait_recv()

        def arrive(count):
            tiles = pl.ds(zz * NY, count)
            arrived(mod_in.at[0, tiles], in_r.at[zz])

            @pl.when(straddle == 1)
            def _():
                arrived(mod_in.at[1, tiles], in2_r.at[zz])

        pl.when(g < 7)(lambda: arrive(NY))
        pl.when(g == 7)(lambda: arrive(NY - 1))
        units = []
        for ky in (2, 3, 1, 0):
            yy = lax.rem(y + ky, NY)
            for e in range(2):
                units.append((yy, e))
        state = []
        for yy, e in units:
            b = 2 * ((yy * NZ + zz) * 2 + x)
            dy0, dx0 = offsets[e][0, b], offsets[e][1, b]
            dy1, dx1 = offsets[e][0, b + 1], offsets[e][1, b + 1]
            left = tab_a[e, dy0] * mask_lo + tab_a[e, dy1] * mask_hi
            image = mod_in[slot_own if e == 0 else slot_par, zz * NY + yy]
            blurred = jnp.dot(left, split(image), preferred_element_type=F32).astype(BF16)
            state.append([yy, e, b, dy0, dy1, dx0, dx1, blurred])
        for s in state:
            yy, e, b, dy0, dy1, dx0, dx1, blurred = s
            right = jnp.concatenate([tab_r[e, dx0] * mask_lo, tab_r[e, dx1] * mask_hi], axis=0)
            predicted = lax.dot_general(blurred, right, (((1,), (1,)), ((), ())), preferred_element_type=F32)
            seen = (obs_st[x, zz, yy] if e == 0 else obs_in[zz, yy]).astype(F32)
            scale = jnp.where(low[:1], scales[e][0, b], scales[e][0, b + 1])
            s.append((scale * (predicted - seen)).astype(BF16))
        for s in state:
            yy, e, b, dy0, dy1, dx0, dx1, blurred, misfit = s
            left_t = tab_at[e, dy0] * mask_lo + tab_at[e, dy1] * mask_hi
            s.append(jnp.dot(left_t, split(misfit), preferred_element_type=F32).astype(BF16))
        terms = {}
        for s in state:
            yy, e, b, dy0, dy1, dx0, dx1, blurred, misfit, back = s
            right = jnp.concatenate([tab_r[e, dx0] * mask_lo, tab_r[e, dx1] * mask_hi], axis=0)
            terms.setdefault(len(terms) if e == 0 else len(terms) - 1, [yy]).append(
                jnp.dot(back, right, preferred_element_type=F32)
            )
        for yy, own, par in terms.values():
            zero = jnp.zeros_like(own)
            term_out[zz * NY + yy] = (jnp.where(own_first, own, zero) + jnp.where(par_first, par, zero)).astype(BF16)
            term_out2[zz * NY + yy] = (jnp.where(own_first, zero, own) + jnp.where(par_first, zero, par)).astype(BF16)
        for ky in (2, 3, 1, 0):
            yy = lax.rem(y + ky, NY)

            def ship():
                term_copy(yy, zz).start()

                @pl.when(straddle == 1)
                def _():
                    term2_copy(yy, zz).start()

            if ky == 0:
                pl.when(g < 7)(ship)
            else:
                ship()
        return carry

    lax.fori_loop(0, 8, group, 0)

    term_in[z * NY + y] = term_out[z * NY + y]

    @pl.when(straddle == 1)
    def _():
        term_in2[straddle_id] = term_out2[z * NY + y]

    send_mats.wait_send()
    send_off.wait_send()
    send_scale.wait_send()
    arrived(obs_in, obs_s)
    arrived(mod_in.at[0, pl.ds(0, 31)], in_s)
    for i, (ys, zs) in enumerate(STRADDLERS):

        @pl.when(jnp.logical_not(jnp.logical_and(y == ys, z == zs)))
        def _():
            arrived(models_low.at[0], in2_s.at[i])

    arrived(term_in.at[pl.ds(0, 31)], t_r)
    for i, (ys, zs) in enumerate(STRADDLERS):

        @pl.when(jnp.logical_not(jnp.logical_and(y == ys, z == zs)))
        def _():
            arrived(term_in2.at[i], t2_r.at[i])

    seen_by = jnp.where(even, counts[0, 0].astype(F32), counts[0, 1].astype(F32))
    factor = step_size / seen_by
    for c in range(BANDS):
        total = jnp.zeros((CUT, 128), F32)
        for yy in range(NY):
            for zz in range(NZ):
                if band_of((yy * NZ + zz) * 2) == c:
                    total = total + term_in[zz * NY + yy].astype(F32)
        for i, (ys, zs) in enumerate(STRADDLERS):
            if band_of((ys * NZ + zs) * 2 + 1) == c:
                total = total + term_in2[i].astype(F32)
        out[c] = factor * swap(total)
        pltpu.make_async_copy(out.at[c], out_h.at[c], out_sem).start()

    arrived(term_out.at[pl.ds(0, 31)], t_s)

    @pl.when(straddle == 1)
    def _():
        arrived(term_out2.at[pl.ds(0, 31)], t2_s)

    arrived(out, out_sem)


def on_device(
    models, observed, weights, coverage, offsets, counts, psf_y, resample_y, psf_x, resample_x
):
    pair_models = models[0].reshape(2, BANDS, 32, 128).transpose(1, 2, 0, 3).reshape(BANDS, CUT, 128)
    blocks = observed[0].reshape(16, 8, 32, 128).transpose(0, 2, 1, 3).reshape(16, 256, 128)
    dma = pltpu.SemaphoreType.DMA
    change = pl.pallas_call(
        kernel,
        out_shape=jax.ShapeDtypeStruct((BANDS, CUT, 128), F32),
        in_specs=[pl.BlockSpec(memory_space=pltpu.HBM)] * 10,
        out_specs=pl.BlockSpec(memory_space=pl.ANY),
        scratch_shapes=[
            pltpu.VMEM((BANDS, CUT, 128), F32),
            pltpu.VMEM((BANDS, CUT, 128), F32),
            pltpu.VMEM((1, 128), F32),
            pltpu.VMEM((1, 128), jnp.int32),
            pltpu.VMEM((2, 128), jnp.int32),
            pltpu.SMEM((1, 2), jnp.int32),
            pltpu.VMEM((1, PIX2), BF16),
            pltpu.VMEM((1, PIX2), BF16),
            pltpu.VMEM((1, PIX2), BF16),
            pltpu.VMEM((1, PIX2), BF16),
            pltpu.VMEM((16, 256, 128), BF16),
            pltpu.VMEM((2, NZ, NY, CUT, 128), BF16),
            pltpu.VMEM((NZ, NY, CUT, 128), BF16),
            pltpu.VMEM((BANDS, CUT, 128), BF16),
            pltpu.VMEM((2, NZ * NY, CUT, 128), BF16),
            pltpu.VMEM((NZ * NY, CUT, 128), BF16),
            pltpu.VMEM((NZ * NY, CUT, 128), BF16),
            pltpu.VMEM((NZ * NY, CUT, 128), BF16),
            pltpu.VMEM((len(STRADDLERS), CUT, 128), BF16),
            pltpu.VMEM((2, CUT, 128), BF16),
            pltpu.VMEM((2, CUT, 128), BF16),
            pltpu.VMEM((2, CUT, CUT, 128), BF16),
            pltpu.VMEM((2, CUT, CUT, 128), BF16),
            pltpu.VMEM((2, CUT, CUT, 128), BF16),
            pltpu.VMEM((32, 128), F32),
            pltpu.VMEM((CUT, 128), F32),
            pltpu.VMEM((128, 128), F32),
            pltpu.VMEM((256, 128), F32),
            pltpu.VMEM((1, 128), F32),
            pltpu.VMEM((1, 128), F32),
            pltpu.VMEM((2, 128), jnp.int32),
            pltpu.SMEM((2, 128), jnp.int32),
            pltpu.SMEM((2, 128), jnp.int32),
            pltpu.SMEM((1, 128), F32),
            pltpu.SMEM((1, 128), F32),
            dma, dma((NZ,)), dma((2,)), dma((NZ,)), dma, dma((NZ,)),
            dma, dma, dma, dma((2,)), dma((3,)), dma((3,)), dma((14,)), dma,
        ],
        compiler_params=pltpu.CompilerParams(
            collective_id=0, has_side_effects=True, vmem_limit_bytes=60_000_000
        ),
    )(
        pair_models, blocks, weights, coverage, offsets[0].T, counts, psf_y, resample_y, psf_x, resample_x
    )
    updated = pair_models - change
    return updated.reshape(BANDS, 32, 2, 128).transpose(2, 0, 1, 3).reshape(1, 2, BANDS, PIX2)


def solution(mesh):
    return jax.shard_map(
        on_device,
        mesh=mesh,
        in_specs=(
            P("blend", "epoch", None, None),
            P("epoch", "blend", None),
            P("epoch", "blend"),
            P("epoch", "blend"),
            P("epoch", "blend", None),
            P("blend", "epoch"),
            P("epoch", None),
            P("epoch", None),
            P("epoch", None),
            P("epoch", None),
        ),
        out_specs=P("blend", "epoch", None, None),
        check_vma=False,
    )
```

```python
import functools

import jax
import jax.numpy as jnp
from jax import lax
from jax.experimental import pallas as pl
from jax.experimental.pallas import tpu as pltpu
from jax.sharding import PartitionSpec as P

CUT = 64
BANDS = 6
PIX2 = 4096
E = 64
NY, NZ = 4, 8
KY = (2, 3, 1, 0)
ORDER = (5, 3, 4, 6, 2, 7, 1, 0)
step_size = 0.5
MESH = pl.DeviceIdType.MESH
F32, BF16 = jnp.float32, jnp.bfloat16


def band_of(epoch):
    return epoch * BANDS // E


STRADDLERS = [
    (y, z) for y in range(NY) for z in range(NZ) if band_of((y * NZ + z) * 2) != band_of((y * NZ + z) * 2 + 1)
]


def kernel(
    models_h, obs_hbm, weights_h, coverage_h, offs_h, counts_h, psf_y_h, res_y_h, psf_x_h, res_x_h, out_h,
    out, models, weights, coverage, offs, counts, psf_y, res_y, psf_x, res_x, obs_v, obs_st, obs_in, models_low, mod_in, term_out, term_out2, term_in, term_in2,
    mats, mats_in, tab_a, tab_at, tab_r, fold, rows_f, wide, spread,
    scale_v, scale_in, offs_in, off_own, off_par, sc_own, sc_par,
    in_s, in_r, in2_s, in2_r, obs_s, obs_r, t_s, t_r, t2_s, t2_r, small_s, small_r, local, out_sem,
):
    me = lax.axis_index("epoch")
    x = lax.rem(me, 2)
    z = lax.rem(lax.div(me, 2), NZ)
    y = lax.div(me, 2 * NZ)
    partner = me + 1 - 2 * x

    def device(yy, zz):
        return (yy * NZ + zz) * 2 + x

    def place(ky, kz):
        return lax.rem(y + ky, NY), lax.rem(z + kz, NZ)

    relative = [(ky, kz) for kz in ORDER for ky in KY]
    others = [r for r in relative if r != (0, 0)]

    def remote(src, dst, send, recv, target):
        return pltpu.make_async_remote_copy(
            src_ref=src, dst_ref=dst, send_sem=send, recv_sem=recv, device_id={"epoch": target}, device_id_type=MESH
        )

    barrier = pltpu.get_barrier_semaphore()
    pl.semaphore_signal(barrier, inc=1, device_id={"epoch": partner}, device_id_type=MESH)
    for ky, kz in others:
        pl.semaphore_signal(barrier, inc=1, device_id={"epoch": device(*place(ky, kz))}, device_id_type=MESH)

    mat_loads = [
        pltpu.make_async_copy(src, dst, local.at[6 + i])
        for i, (src, dst) in enumerate(((psf_y_h, psf_y), (res_y_h, res_y), (psf_x_h, psf_x), (res_x_h, res_x)))
    ]
    load_models = pltpu.make_async_copy(models_h, models, local.at[5])
    load_obs = pltpu.make_async_copy(obs_hbm, obs_v, local.at[0])
    load_off = pltpu.make_async_copy(offs_h, off_own, local.at[1])
    small_loads = [
        pltpu.make_async_copy(src, dst, local.at[10 + i])
        for i, (src, dst) in enumerate(
            ((weights_h, weights), (coverage_h, coverage), (offs_h, offs), (counts_h, counts))
        )
    ]
    load_models.start()
    for load in mat_loads + [load_off] + small_loads:
        load.start()

    straddle = jnp.int32(0)
    straddle_id = jnp.int32(0)
    for i, (ys, zs) in enumerate(STRADDLERS):
        hit = jnp.where(jnp.logical_and(y == ys, z == zs), 1, 0).astype(jnp.int32)
        straddle = straddle + hit
        straddle_id = straddle_id + i * hit

    lane = lax.broadcasted_iota(jnp.int32, (CUT, 128), 1)
    row = lax.broadcasted_iota(jnp.int32, (CUT, 128), 0)
    low = lane < CUT
    low_half = low[:32]
    even = lax.rem(row, 2) == 0
    mask_lo = jnp.where(low, 1.0, 0.0).astype(BF16)
    mask_hi = jnp.where(low, 0.0, 1.0).astype(BF16)

    def swap(v):
        turned = pltpu.roll(v, CUT, 1)
        up = pltpu.roll(turned, CUT - 1, 0)
        down = pltpu.roll(turned, 1, 0)
        return jnp.where(low, jnp.where(even, v, down), jnp.where(even, up, v))

    def unfold(ref):
        v = ref[...].astype(F32)
        for k in range(32):
            fold[k : k + 1, :] = v[:, k * 128 : (k + 1) * 128]
        top = fold[...]
        return top, pltpu.roll(top, CUT, 1)

    def natural(ref):
        top, bottom = unfold(ref)
        rows_f[pl.ds(0, 32, stride=2), :] = top
        rows_f[pl.ds(1, 32, stride=2), :] = bottom
        return rows_f[...]

    def doubled(v):
        return jnp.where(low, v, pltpu.roll(v, CUT, 1))

    load_models.wait()
    load_obs.start()
    for c in range(BANDS):
        models_low[c] = swap(models[c]).astype(BF16)

    def tables(slot, source):
        left = source[0].astype(F32)
        right = source[1].astype(F32)
        wide[...] = jnp.concatenate([left, left], axis=0).T

        def one(d, carry):
            tab_a[slot, d] = pltpu.roll(left, d, 1).astype(BF16)
            tab_at[slot, d] = wide[pl.ds(CUT - d, CUT), :].astype(BF16)
            tab_r[slot, d] = pltpu.roll(right, d, 1).astype(BF16)
            return carry

        lax.fori_loop(0, CUT, one, 0, unroll=4)

    pl.semaphore_wait(barrier, 32)

    def turn(g):
        kz = jnp.int32(ORDER[0])
        for i in range(1, NZ):
            kz = jnp.where(g == i, ORDER[i], kz)
        return kz

    def model_copy(ky, kz):
        yy, zz = place(ky, kz)
        band = lax.div((yy * NZ + zz) * 2 * BANDS, E)
        return remote(
            models_low.at[band], mod_in.at[0, z * NY + y], in_s, in_r.at[z], device(yy, zz)
        )

    for i, (ys, zs) in enumerate(STRADDLERS):
        band = band_of((ys * NZ + zs) * 2 + 1)
        here = jnp.logical_and(y == ys, z == zs)

        @pl.when(jnp.logical_not(here))
        def _():
            remote(
                models_low.at[band], mod_in.at[1, z * NY + y], in2_s.at[i], in2_r.at[z], device(ys, zs)
            ).start()

        @pl.when(here)
        def _():
            mod_in[1, z * NY + y] = models_low[band]

    for ky, kz in others:
        model_copy(ky, kz).start()

    mod_in[0, z * NY + y] = models_low[lax.div((y * NZ + z) * 2 * BANDS, E)]

    for load in mat_loads:
        load.wait()
    top, bottom = unfold(psf_y)
    first = jnp.concatenate([top, bottom], axis=0)[:, :CUT].astype(BF16)
    second = doubled(natural(res_y)).astype(BF16)
    mats[0] = jnp.dot(first, second, preferred_element_type=F32).astype(BF16)
    first = natural(psf_x)[:, :CUT].astype(BF16)
    second = doubled(natural(res_x)).astype(BF16)
    mats[1] = jnp.dot(first, second, preferred_element_type=F32).astype(BF16)

    for load in small_loads:
        load.wait()
    scale_v[...] = weights[...] * coverage[...].astype(F32)
    send_mats = remote(mats, mats_in, small_s.at[0], small_r.at[0], partner)
    send_off = remote(offs, offs_in, small_s.at[1], small_r.at[1], partner)
    send_scale = remote(scale_v, scale_in, small_s.at[2], small_r.at[2], partner)
    send_mats.start()
    send_off.start()
    send_scale.start()
    load_scale = pltpu.make_async_copy(scale_v, sc_own, local.at[2])
    load_scale.start()

    load_obs.wait()

    def relayout(z2):
        def rows(yy, carry):
            spread[...] = obs_v[yy * 4 + z2].astype(F32)
            for s in range(4):
                f0 = spread[pl.ds(2 * s, 32, stride=8), :]
                f1 = spread[pl.ds(2 * s + 1, 32, stride=8), :]
                top = jnp.where(low_half, f0, pltpu.roll(f1, CUT, 1))
                bottom = jnp.where(low_half, pltpu.roll(f0, CUT, 1), f1)
                obs_st[s % 2, 2 * z2 + s // 2, yy] = jnp.concatenate([top, bottom], axis=0).astype(BF16)
            return carry

        lax.fori_loop(0, NY, rows, 0)

    def obs_copy(g):
        zz = lax.rem(z + turn(g), NZ)
        return remote(obs_st.at[1 - x, zz], obs_in.at[zz], obs_s, obs_r.at[g], partner)

    for z2 in range(4):
        relayout(z2)
    for g in range(NZ):
        obs_copy(jnp.int32(g)).start()

    tables(0, mats)
    send_mats.wait_recv()
    tables(1, mats_in)
    send_off.wait_recv()
    send_scale.wait_recv()
    load_off.wait()
    load_scale.wait()
    load_off = pltpu.make_async_copy(offs_in, off_par, local.at[3])
    load_scale = pltpu.make_async_copy(scale_in, sc_par, local.at[4])
    load_off.start()
    load_scale.start()
    load_off.wait()
    load_scale.wait()

    slot_own = straddle * x
    slot_par = straddle * (1 - x)
    own_first = slot_own == 0
    par_first = slot_par == 0
    offsets = (off_own, off_par)
    scales = (sc_own, sc_par)

    def term_copy(yy, zz):
        return remote(
            term_out.at[zz * NY + yy], term_in.at[z * NY + y], t_s, t_r, device(yy, zz)
        )

    def term2_copy(yy, zz):
        return remote(
            term_out2.at[zz * NY + yy], term_in2.at[straddle_id], t2_s, t2_r.at[straddle_id], device(yy, zz)
        )

    def arrived(tiles, semaphore):
        pltpu.make_async_copy(tiles, tiles, semaphore).wait()

    def split(v):
        return jnp.concatenate([v * mask_lo, v * mask_hi], axis=0)

    def group(g, carry):
        kz = turn(g)
        home = kz == 0
        zz = lax.rem(z + kz, NZ)
        obs_copy(g).wait_recv()

        def arrive(count):
            tiles = pl.ds(zz * NY, count)
            arrived(mod_in.at[0, tiles], in_r.at[zz])

            @pl.when(straddle == 1)
            def _():
                arrived(mod_in.at[1, tiles], in2_r.at[zz])

        pl.when(jnp.logical_not(home))(lambda: arrive(NY))
        pl.when(home)(lambda: arrive(NY - 1))
        units = []
        for ky in KY:
            yy = lax.rem(y + ky, NY)
            for e in range(2):
                units.append((yy, e))
        state = []
        for yy, e in units:
            b = 2 * ((yy * NZ + zz) * 2 + x)
            dy0, dx0 = offsets[e][0, b], offsets[e][1, b]
            dy1, dx1 = offsets[e][0, b + 1], offsets[e][1, b + 1]
            left = tab_a[e, dy0] * mask_lo + tab_a[e, dy1] * mask_hi
            image = mod_in[slot_own if e == 0 else slot_par, zz * NY + yy]
            blurred = jnp.dot(left, split(image), preferred_element_type=F32).astype(BF16)
            state.append([yy, e, b, dy0, dy1, dx0, dx1, blurred])
        for s in state:
            yy, e, b, dy0, dy1, dx0, dx1, blurred = s
            right = jnp.concatenate([tab_r[e, dx0] * mask_lo, tab_r[e, dx1] * mask_hi], axis=0)
            predicted = lax.dot_general(blurred, right, (((1,), (1,)), ((), ())), preferred_element_type=F32)
            seen = (obs_st[x, zz, yy] if e == 0 else obs_in[zz, yy]).astype(F32)
            scale = jnp.where(low[:1], scales[e][0, b], scales[e][0, b + 1])
            s.append((scale * (predicted - seen)).astype(BF16))
        for s in state:
            yy, e, b, dy0, dy1, dx0, dx1, blurred, misfit = s
            left_t = tab_at[e, dy0] * mask_lo + tab_at[e, dy1] * mask_hi
            s.append(jnp.dot(left_t, split(misfit), preferred_element_type=F32).astype(BF16))
        terms = {}
        for s in state:
            yy, e, b, dy0, dy1, dx0, dx1, blurred, misfit, back = s
            right = jnp.concatenate([tab_r[e, dx0] * mask_lo, tab_r[e, dx1] * mask_hi], axis=0)
            terms.setdefault(len(terms) if e == 0 else len(terms) - 1, [yy]).append(
                jnp.dot(back, right, preferred_element_type=F32)
            )
        for yy, own, par in terms.values():
            zero = jnp.zeros_like(own)
            term_out[zz * NY + yy] = (jnp.where(own_first, own, zero) + jnp.where(par_first, par, zero)).astype(BF16)
            term_out2[zz * NY + yy] = (jnp.where(own_first, zero, own) + jnp.where(par_first, zero, par)).astype(BF16)
        for ky in KY:
            yy = lax.rem(y + ky, NY)

            def ship():
                term_copy(yy, zz).start()

                @pl.when(straddle == 1)
                def _():
                    term2_copy(yy, zz).start()

            if ky == 0:
                pl.when(jnp.logical_not(home))(ship)
            else:
                ship()
        return carry

    lax.fori_loop(0, 8, group, 0)

    term_in[z * NY + y] = term_out[z * NY + y]

    @pl.when(straddle == 1)
    def _():
        term_in2[straddle_id] = term_out2[z * NY + y]

    send_mats.wait_send()
    send_off.wait_send()
    send_scale.wait_send()
    arrived(obs_in, obs_s)
    arrived(mod_in.at[0, pl.ds(0, 31)], in_s)
    for i, (ys, zs) in enumerate(STRADDLERS):

        @pl.when(jnp.logical_not(jnp.logical_and(y == ys, z == zs)))
        def _():
            arrived(models_low.at[0], in2_s.at[i])

    arrived(term_in.at[pl.ds(0, 31)], t_r)
    for i, (ys, zs) in enumerate(STRADDLERS):

        @pl.when(jnp.logical_not(jnp.logical_and(y == ys, z == zs)))
        def _():
            arrived(term_in2.at[i], t2_r.at[i])

    seen_by = jnp.where(even, counts[0, 0].astype(F32), counts[0, 1].astype(F32))
    factor = step_size / seen_by
    for c in range(BANDS):
        total = jnp.zeros((CUT, 128), F32)
        for yy in range(NY):
            for zz in range(NZ):
                if band_of((yy * NZ + zz) * 2) == c:
                    total = total + term_in[zz * NY + yy].astype(F32)
        for i, (ys, zs) in enumerate(STRADDLERS):
            if band_of((ys * NZ + zs) * 2 + 1) == c:
                total = total + term_in2[i].astype(F32)
        out[c] = factor * swap(total)
        pltpu.make_async_copy(out.at[c], out_h.at[c], out_sem).start()

    arrived(term_out.at[pl.ds(0, 31)], t_s)

    @pl.when(straddle == 1)
    def _():
        arrived(term_out2.at[pl.ds(0, 31)], t2_s)

    arrived(out, out_sem)


def on_device(
    models, observed, weights, coverage, offsets, counts, psf_y, resample_y, psf_x, resample_x
):
    pair_models = models[0].reshape(2, BANDS, 32, 128).transpose(1, 2, 0, 3).reshape(BANDS, CUT, 128)
    blocks = observed[0].reshape(16, 8, 32, 128).transpose(0, 2, 1, 3).reshape(16, 256, 128)
    dma = pltpu.SemaphoreType.DMA
    change = pl.pallas_call(
        kernel,
        out_shape=jax.ShapeDtypeStruct((BANDS, CUT, 128), F32),
        in_specs=[pl.BlockSpec(memory_space=pltpu.HBM)] * 10,
        out_specs=pl.BlockSpec(memory_space=pl.ANY),
        scratch_shapes=[
            pltpu.VMEM((BANDS, CUT, 128), F32),
            pltpu.VMEM((BANDS, CUT, 128), F32),
            pltpu.VMEM((1, 128), F32),
            pltpu.VMEM((1, 128), jnp.int32),
            pltpu.VMEM((2, 128), jnp.int32),
            pltpu.SMEM((1, 2), jnp.int32),
            pltpu.VMEM((1, PIX2), BF16),
            pltpu.VMEM((1, PIX2), BF16),
            pltpu.VMEM((1, PIX2), BF16),
            pltpu.VMEM((1, PIX2), BF16),
            pltpu.VMEM((16, 256, 128), BF16),
            pltpu.VMEM((2, NZ, NY, CUT, 128), BF16),
            pltpu.VMEM((NZ, NY, CUT, 128), BF16),
            pltpu.VMEM((BANDS, CUT, 128), BF16),
            pltpu.VMEM((2, NZ * NY, CUT, 128), BF16),
            pltpu.VMEM((NZ * NY, CUT, 128), BF16),
            pltpu.VMEM((NZ * NY, CUT, 128), BF16),
            pltpu.VMEM((NZ * NY, CUT, 128), BF16),
            pltpu.VMEM((len(STRADDLERS), CUT, 128), BF16),
            pltpu.VMEM((2, CUT, 128), BF16),
            pltpu.VMEM((2, CUT, 128), BF16),
            pltpu.VMEM((2, CUT, CUT, 128), BF16),
            pltpu.VMEM((2, CUT, CUT, 128), BF16),
            pltpu.VMEM((2, CUT, CUT, 128), BF16),
            pltpu.VMEM((32, 128), F32),
            pltpu.VMEM((CUT, 128), F32),
            pltpu.VMEM((128, 128), F32),
            pltpu.VMEM((256, 128), F32),
            pltpu.VMEM((1, 128), F32),
            pltpu.VMEM((1, 128), F32),
            pltpu.VMEM((2, 128), jnp.int32),
            pltpu.SMEM((2, 128), jnp.int32),
            pltpu.SMEM((2, 128), jnp.int32),
            pltpu.SMEM((1, 128), F32),
            pltpu.SMEM((1, 128), F32),
            dma, dma((NZ,)), dma((2,)), dma((NZ,)), dma, dma((NZ,)),
            dma, dma, dma, dma((2,)), dma((3,)), dma((3,)), dma((14,)), dma,
        ],
        compiler_params=pltpu.CompilerParams(
            collective_id=0, has_side_effects=True, vmem_limit_bytes=60_000_000
        ),
    )(
        pair_models, blocks, weights, coverage, offsets[0].T, counts, psf_y, resample_y, psf_x, resample_x
    )
    updated = pair_models - change
    return updated.reshape(BANDS, 32, 2, 128).transpose(2, 0, 1, 3).reshape(1, 2, BANDS, PIX2)


def solution(mesh):
    return jax.shard_map(
        on_device,
        mesh=mesh,
        in_specs=(
            P("blend", "epoch", None, None),
            P("epoch", "blend", None),
            P("epoch", "blend"),
            P("epoch", "blend"),
            P("epoch", "blend", None),
            P("blend", "epoch"),
            P("epoch", None),
            P("epoch", None),
            P("epoch", None),
            P("epoch", None),
        ),
        out_specs=P("blend", "epoch", None, None),
        check_vma=False,
    )
```

```python
import functools

import jax
import jax.numpy as jnp
from jax import lax
from jax.experimental import pallas as pl
from jax.experimental.pallas import tpu as pltpu
from jax.sharding import PartitionSpec as P

CUT = 64
BANDS = 6
PIX2 = 4096
E = 64
NY, NZ = 4, 8
KY = (2, 3, 1, 0)
ORDER = (5, 3, 4, 6, 2, 7, 1, 0)
step_size = 0.5
MESH = pl.DeviceIdType.MESH
F32, BF16 = jnp.float32, jnp.bfloat16


def band_of(epoch):
    return epoch * BANDS // E


STRADDLERS = [
    (y, z) for y in range(NY) for z in range(NZ) if band_of((y * NZ + z) * 2) != band_of((y * NZ + z) * 2 + 1)
]


def swap(v):
    low = lax.broadcasted_iota(jnp.int32, (CUT, 128), 1) < CUT
    even = lax.rem(lax.broadcasted_iota(jnp.int32, (CUT, 128), 0), 2) == 0
    turned = pltpu.roll(v, CUT, 1)
    up = pltpu.roll(turned, CUT - 1, 0)
    down = pltpu.roll(turned, 1, 0)
    return jnp.where(low, jnp.where(even, v, down), jnp.where(even, up, v))


def finish(models_h, terms_h, terms2_h, counts_h, updated_h, models, terms, terms2, counts, updated, sems):
    loads = [
        pltpu.make_async_copy(src, dst, sems.at[i])
        for i, (src, dst) in enumerate(
            ((counts_h, counts), (terms2_h, terms2), (terms_h, terms), (models_h, models))
        )
    ]
    for load in loads:
        load.start()
    for load in loads:
        load.wait()
    even = lax.rem(lax.broadcasted_iota(jnp.int32, (CUT, 128), 0), 2) == 0
    seen_by = jnp.where(even, counts[0, 0].astype(F32), counts[0, 1].astype(F32))
    factor = step_size / seen_by
    for c in range(BANDS):
        total = jnp.zeros((CUT, 128), F32)
        for yy in range(NY):
            for zz in range(NZ):
                if band_of((yy * NZ + zz) * 2) == c:
                    total = total + terms[zz * NY + yy].astype(F32)
        for i, (ys, zs) in enumerate(STRADDLERS):
            if band_of((ys * NZ + zs) * 2 + 1) == c:
                total = total + terms2[i].astype(F32)
        updated[c] = models[c] - factor * swap(total)
        pltpu.make_async_copy(updated.at[c], updated_h.at[c], sems.at[4]).start()
    pltpu.make_async_copy(updated, updated_h, sems.at[4]).wait()


def kernel(
    models_h, obs_hbm, weights_h, coverage_h, offs_h, psf_y_h, res_y_h, psf_x_h, res_x_h, term_in, term_in2,
    models, weights, coverage, offs, psf_y, res_y, psf_x, res_x, obs_v, obs_st, obs_in, models_low, mod_in, term_out, term_out2,
    mats, mats_in, tab_a, tab_at, tab_r, fold, rows_f, wide, spread,
    scale_v, scale_in, offs_in, off_own, off_par, sc_own, sc_par,
    in_s, in_r, in2_s, in2_r, obs_s, obs_r, t_s, t_r, t2_s, t2_r, small_s, small_r, local, home_sem,
):
    me = lax.axis_index("epoch")
    x = lax.rem(me, 2)
    z = lax.rem(lax.div(me, 2), NZ)
    y = lax.div(me, 2 * NZ)
    partner = me + 1 - 2 * x

    def device(yy, zz):
        return (yy * NZ + zz) * 2 + x

    def place(ky, kz):
        return lax.rem(y + ky, NY), lax.rem(z + kz, NZ)

    relative = [(ky, kz) for kz in ORDER for ky in KY]
    others = [r for r in relative if r != (0, 0)]

    def remote(src, dst, send, recv, target):
        return pltpu.make_async_remote_copy(
            src_ref=src, dst_ref=dst, send_sem=send, recv_sem=recv, device_id={"epoch": target}, device_id_type=MESH
        )

    barrier = pltpu.get_barrier_semaphore()
    pl.semaphore_signal(barrier, inc=1, device_id={"epoch": partner}, device_id_type=MESH)
    for ky, kz in others:
        pl.semaphore_signal(barrier, inc=1, device_id={"epoch": device(*place(ky, kz))}, device_id_type=MESH)

    mat_loads = [
        pltpu.make_async_copy(src, dst, local.at[6 + i])
        for i, (src, dst) in enumerate(((psf_y_h, psf_y), (res_y_h, res_y), (psf_x_h, psf_x), (res_x_h, res_x)))
    ]
    load_models = pltpu.make_async_copy(models_h, models, local.at[5])
    load_obs = pltpu.make_async_copy(obs_hbm, obs_v, local.at[0])
    load_off = pltpu.make_async_copy(offs_h, off_own, local.at[1])
    small_loads = [
        pltpu.make_async_copy(src, dst, local.at[10 + i])
        for i, (src, dst) in enumerate(
            ((weights_h, weights), (coverage_h, coverage), (offs_h, offs))
        )
    ]
    load_models.start()
    for load in mat_loads + [load_off] + small_loads:
        load.start()

    straddle = jnp.int32(0)
    straddle_id = jnp.int32(0)
    for i, (ys, zs) in enumerate(STRADDLERS):
        hit = jnp.where(jnp.logical_and(y == ys, z == zs), 1, 0).astype(jnp.int32)
        straddle = straddle + hit
        straddle_id = straddle_id + i * hit

    lane = lax.broadcasted_iota(jnp.int32, (CUT, 128), 1)
    row = lax.broadcasted_iota(jnp.int32, (CUT, 128), 0)
    low = lane < CUT
    low_half = low[:32]
    even = lax.rem(row, 2) == 0
    mask_lo = jnp.where(low, 1.0, 0.0).astype(BF16)
    mask_hi = jnp.where(low, 0.0, 1.0).astype(BF16)

    def unfold(ref):
        v = ref[...].astype(F32)
        for k in range(32):
            fold[k : k + 1, :] = v[:, k * 128 : (k + 1) * 128]
        top = fold[...]
        return top, pltpu.roll(top, CUT, 1)

    def natural(ref):
        top, bottom = unfold(ref)
        rows_f[pl.ds(0, 32, stride=2), :] = top
        rows_f[pl.ds(1, 32, stride=2), :] = bottom
        return rows_f[...]

    def doubled(v):
        return jnp.where(low, v, pltpu.roll(v, CUT, 1))

    load_models.wait()
    load_obs.start()
    for c in range(BANDS):
        models_low[c] = swap(models[c]).astype(BF16)

    def tables(slot, source):
        left = source[0].astype(F32)
        right = source[1].astype(F32)
        wide[...] = jnp.concatenate([left, left], axis=0).T

        def one(d, carry):
            tab_a[slot, d] = pltpu.roll(left, d, 1).astype(BF16)
            tab_at[slot, d] = wide[pl.ds(CUT - d, CUT), :].astype(BF16)
            tab_r[slot, d] = pltpu.roll(right, d, 1).astype(BF16)
            return carry

        lax.fori_loop(0, CUT, one, 0, unroll=4)

    pl.semaphore_wait(barrier, 32)

    def turn(g):
        kz = jnp.int32(ORDER[0])
        for i in range(1, NZ):
            kz = jnp.where(g == i, ORDER[i], kz)
        return kz

    def model_copy(ky, kz):
        yy, zz = place(ky, kz)
        band = lax.div((yy * NZ + zz) * 2 * BANDS, E)
        return remote(
            models_low.at[band], mod_in.at[0, z * NY + y], in_s, in_r.at[z], device(yy, zz)
        )

    for i, (ys, zs) in enumerate(STRADDLERS):
        band = band_of((ys * NZ + zs) * 2 + 1)
        here = jnp.logical_and(y == ys, z == zs)

        @pl.when(jnp.logical_not(here))
        def _():
            remote(
                models_low.at[band], mod_in.at[1, z * NY + y], in2_s.at[i], in2_r.at[z], device(ys, zs)
            ).start()

        @pl.when(here)
        def _():
            mod_in[1, z * NY + y] = models_low[band]

    for ky, kz in others:
        model_copy(ky, kz).start()

    mod_in[0, z * NY + y] = models_low[lax.div((y * NZ + z) * 2 * BANDS, E)]

    for load in mat_loads:
        load.wait()
    top, bottom = unfold(psf_y)
    first = jnp.concatenate([top, bottom], axis=0)[:, :CUT].astype(BF16)
    second = doubled(natural(res_y)).astype(BF16)
    mats[0] = jnp.dot(first, second, preferred_element_type=F32).astype(BF16)
    first = natural(psf_x)[:, :CUT].astype(BF16)
    second = doubled(natural(res_x)).astype(BF16)
    mats[1] = jnp.dot(first, second, preferred_element_type=F32).astype(BF16)

    for load in small_loads:
        load.wait()
    scale_v[...] = weights[...] * coverage[...].astype(F32)
    send_mats = remote(mats, mats_in, small_s.at[0], small_r.at[0], partner)
    send_off = remote(offs, offs_in, small_s.at[1], small_r.at[1], partner)
    send_scale = remote(scale_v, scale_in, small_s.at[2], small_r.at[2], partner)
    send_mats.start()
    send_off.start()
    send_scale.start()
    load_scale = pltpu.make_async_copy(scale_v, sc_own, local.at[2])
    load_scale.start()

    load_obs.wait()

    def relayout(z2):
        def rows(yy, carry):
            spread[...] = obs_v[yy * 4 + z2].astype(F32)
            for s in range(4):
                f0 = spread[pl.ds(2 * s, 32, stride=8), :]
                f1 = spread[pl.ds(2 * s + 1, 32, stride=8), :]
                top = jnp.where(low_half, f0, pltpu.roll(f1, CUT, 1))
                bottom = jnp.where(low_half, pltpu.roll(f0, CUT, 1), f1)
                obs_st[s % 2, 2 * z2 + s // 2, yy] = jnp.concatenate([top, bottom], axis=0).astype(BF16)
            return carry

        lax.fori_loop(0, NY, rows, 0)

    def obs_copy(g):
        zz = lax.rem(z + turn(g), NZ)
        return remote(obs_st.at[1 - x, zz], obs_in.at[zz], obs_s, obs_r.at[g], partner)

    for z2 in range(4):
        relayout(z2)
    for g in range(NZ):
        obs_copy(jnp.int32(g)).start()

    tables(0, mats)
    send_mats.wait_recv()
    tables(1, mats_in)
    send_off.wait_recv()
    send_scale.wait_recv()
    load_off.wait()
    load_scale.wait()
    load_off = pltpu.make_async_copy(offs_in, off_par, local.at[3])
    load_scale = pltpu.make_async_copy(scale_in, sc_par, local.at[4])
    load_off.start()
    load_scale.start()
    load_off.wait()
    load_scale.wait()

    slot_own = straddle * x
    slot_par = straddle * (1 - x)
    own_first = slot_own == 0
    par_first = slot_par == 0
    offsets = (off_own, off_par)
    scales = (sc_own, sc_par)

    def term_copy(yy, zz):
        return remote(
            term_out.at[zz * NY + yy], term_in.at[z * NY + y], t_s, t_r, device(yy, zz)
        )

    def term2_copy(yy, zz):
        return remote(
            term_out2.at[zz * NY + yy], term_in2.at[straddle_id], t2_s, t2_r.at[straddle_id], device(yy, zz)
        )

    def arrived(tiles, semaphore):
        pltpu.make_async_copy(tiles, tiles, semaphore).wait()

    def split(v):
        return jnp.concatenate([v * mask_lo, v * mask_hi], axis=0)

    def group(g, carry):
        kz = turn(g)
        home = kz == 0
        zz = lax.rem(z + kz, NZ)
        obs_copy(g).wait_recv()

        def arrive(count):
            tiles = pl.ds(zz * NY, count)
            arrived(mod_in.at[0, tiles], in_r.at[zz])

            @pl.when(straddle == 1)
            def _():
                arrived(mod_in.at[1, tiles], in2_r.at[zz])

        pl.when(jnp.logical_not(home))(lambda: arrive(NY))
        pl.when(home)(lambda: arrive(NY - 1))
        units = []
        for ky in KY:
            yy = lax.rem(y + ky, NY)
            for e in range(2):
                units.append((yy, e))
        state = []
        for yy, e in units:
            b = 2 * ((yy * NZ + zz) * 2 + x)
            dy0, dx0 = offsets[e][0, b], offsets[e][1, b]
            dy1, dx1 = offsets[e][0, b + 1], offsets[e][1, b + 1]
            left = tab_a[e, dy0] * mask_lo + tab_a[e, dy1] * mask_hi
            image = mod_in[slot_own if e == 0 else slot_par, zz * NY + yy]
            blurred = jnp.dot(left, split(image), preferred_element_type=F32).astype(BF16)
            state.append([yy, e, b, dy0, dy1, dx0, dx1, blurred])
        for s in state:
            yy, e, b, dy0, dy1, dx0, dx1, blurred = s
            right = jnp.concatenate([tab_r[e, dx0] * mask_lo, tab_r[e, dx1] * mask_hi], axis=0)
            predicted = lax.dot_general(blurred, right, (((1,), (1,)), ((), ())), preferred_element_type=F32)
            seen = (obs_st[x, zz, yy] if e == 0 else obs_in[zz, yy]).astype(F32)
            scale = jnp.where(low[:1], scales[e][0, b], scales[e][0, b + 1])
            s.append((scale * (predicted - seen)).astype(BF16))
        for s in state:
            yy, e, b, dy0, dy1, dx0, dx1, blurred, misfit = s
            left_t = tab_at[e, dy0] * mask_lo + tab_at[e, dy1] * mask_hi
            s.append(jnp.dot(left_t, split(misfit), preferred_element_type=F32).astype(BF16))
        terms = {}
        for s in state:
            yy, e, b, dy0, dy1, dx0, dx1, blurred, misfit, back = s
            right = jnp.concatenate([tab_r[e, dx0] * mask_lo, tab_r[e, dx1] * mask_hi], axis=0)
            terms.setdefault(len(terms) if e == 0 else len(terms) - 1, [yy]).append(
                jnp.dot(back, right, preferred_element_type=F32)
            )
        for yy, own, par in terms.values():
            zero = jnp.zeros_like(own)
            term_out[zz * NY + yy] = (jnp.where(own_first, own, zero) + jnp.where(par_first, par, zero)).astype(BF16)
            term_out2[zz * NY + yy] = (jnp.where(own_first, zero, own) + jnp.where(par_first, zero, par)).astype(BF16)
        for ky in KY:
            yy = lax.rem(y + ky, NY)

            def ship():
                term_copy(yy, zz).start()

                @pl.when(straddle == 1)
                def _():
                    term2_copy(yy, zz).start()

            if ky == 0:
                pl.when(jnp.logical_not(home))(ship)
            else:
                ship()
        return carry

    lax.fori_loop(0, 8, group, 0)

    home = z * NY + y
    pltpu.make_async_copy(term_out.at[home], term_in.at[home], home_sem.at[0]).start()

    @pl.when(straddle == 1)
    def _():
        pltpu.make_async_copy(term_out2.at[home], term_in2.at[straddle_id], home_sem.at[1]).start()

    send_mats.wait_send()
    send_off.wait_send()
    send_scale.wait_send()
    arrived(obs_in, obs_s)
    arrived(mod_in.at[0, pl.ds(0, 31)], in_s)
    for i, (ys, zs) in enumerate(STRADDLERS):

        @pl.when(jnp.logical_not(jnp.logical_and(y == ys, z == zs)))
        def _():
            arrived(models_low.at[0], in2_s.at[i])

    arrived(term_in.at[pl.ds(0, 31)], t_r)
    for i, (ys, zs) in enumerate(STRADDLERS):

        @pl.when(jnp.logical_not(jnp.logical_and(y == ys, z == zs)))
        def _():
            arrived(term_in2.at[i], t2_r.at[i])

    arrived(term_in.at[0], home_sem.at[0])
    arrived(term_out.at[pl.ds(0, 31)], t_s)

    @pl.when(straddle == 1)
    def _():
        arrived(term_out2.at[pl.ds(0, 31)], t2_s)
        arrived(term_in2.at[0], home_sem.at[1])


def on_device(
    models, observed, weights, coverage, offsets, counts, psf_y, resample_y, psf_x, resample_x
):
    pair_models = models[0].reshape(2, BANDS, 32, 128).transpose(1, 2, 0, 3).reshape(BANDS, CUT, 128)
    blocks = observed[0].reshape(16, 8, 32, 128).transpose(0, 2, 1, 3).reshape(16, 256, 128)
    anywhere = pl.BlockSpec(memory_space=pl.ANY)
    dma = pltpu.SemaphoreType.DMA
    terms, terms2 = pl.pallas_call(
        kernel,
        out_shape=(
            jax.ShapeDtypeStruct((NZ * NY, CUT, 128), BF16),
            jax.ShapeDtypeStruct((len(STRADDLERS), CUT, 128), BF16),
        ),
        in_specs=[anywhere] * 9,
        out_specs=(anywhere, anywhere),
        scratch_shapes=[
            pltpu.VMEM((BANDS, CUT, 128), F32),
            pltpu.VMEM((1, 128), F32),
            pltpu.VMEM((1, 128), jnp.int32),
            pltpu.VMEM((2, 128), jnp.int32),
            pltpu.VMEM((1, PIX2), BF16),
            pltpu.VMEM((1, PIX2), BF16),
            pltpu.VMEM((1, PIX2), BF16),
            pltpu.VMEM((1, PIX2), BF16),
            pltpu.VMEM((16, 256, 128), BF16),
            pltpu.VMEM((2, NZ, NY, CUT, 128), BF16),
            pltpu.VMEM((NZ, NY, CUT, 128), BF16),
            pltpu.VMEM((BANDS, CUT, 128), BF16),
            pltpu.VMEM((2, NZ * NY, CUT, 128), BF16),
            pltpu.VMEM((NZ * NY, CUT, 128), BF16),
            pltpu.VMEM((NZ * NY, CUT, 128), BF16),
            pltpu.VMEM((2, CUT, 128), BF16),
            pltpu.VMEM((2, CUT, 128), BF16),
            pltpu.VMEM((2, CUT, CUT, 128), BF16),
            pltpu.VMEM((2, CUT, CUT, 128), BF16),
            pltpu.VMEM((2, CUT, CUT, 128), BF16),
            pltpu.VMEM((32, 128), F32),
            pltpu.VMEM((CUT, 128), F32),
            pltpu.VMEM((128, 128), F32),
            pltpu.VMEM((256, 128), F32),
            pltpu.VMEM((1, 128), F32),
            pltpu.VMEM((1, 128), F32),
            pltpu.VMEM((2, 128), jnp.int32),
            pltpu.SMEM((2, 128), jnp.int32),
            pltpu.SMEM((2, 128), jnp.int32),
            pltpu.SMEM((1, 128), F32),
            pltpu.SMEM((1, 128), F32),
            dma, dma((NZ,)), dma((2,)), dma((NZ,)), dma, dma((NZ,)),
            dma, dma, dma, dma((2,)), dma((3,)), dma((3,)), dma((13,)), dma((2,)),
        ],
        compiler_params=pltpu.CompilerParams(
            collective_id=0, has_side_effects=True, vmem_limit_bytes=60_000_000
        ),
    )(
        pair_models, blocks, weights, coverage, offsets[0].T, psf_y, resample_y, psf_x, resample_x
    )
    updated = pl.pallas_call(
        finish,
        out_shape=jax.ShapeDtypeStruct((BANDS, CUT, 128), F32),
        in_specs=[anywhere] * 4,
        out_specs=anywhere,
        scratch_shapes=[
            pltpu.VMEM((BANDS, CUT, 128), F32),
            pltpu.VMEM((NZ * NY, CUT, 128), BF16),
            pltpu.VMEM((len(STRADDLERS), CUT, 128), BF16),
            pltpu.SMEM((1, 2), jnp.int32),
            pltpu.VMEM((BANDS, CUT, 128), F32),
            dma((5,)),
        ],
        compiler_params=pltpu.CompilerParams(vmem_limit_bytes=60_000_000),
    )(pair_models, terms, terms2, counts)
    return updated.reshape(BANDS, 32, 2, 128).transpose(2, 0, 1, 3).reshape(1, 2, BANDS, PIX2)


def solution(mesh):
    return jax.shard_map(
        on_device,
        mesh=mesh,
        in_specs=(
            P("blend", "epoch", None, None),
            P("epoch", "blend", None),
            P("epoch", "blend"),
            P("epoch", "blend"),
            P("epoch", "blend", None),
            P("blend", "epoch"),
            P("epoch", None),
            P("epoch", None),
            P("epoch", None),
            P("epoch", None),
        ),
        out_specs=P("blend", "epoch", None, None),
        check_vma=False,
    )
```

```python
import functools

import jax
import jax.numpy as jnp
from jax import lax
from jax.experimental import pallas as pl
from jax.experimental.pallas import tpu as pltpu
from jax.sharding import PartitionSpec as P

CUT = 64
BANDS = 6
PIX2 = 4096
E = 64
NY, NZ = 4, 8
KY = (2, 3, 1, 0)
ORDER = (5, 3, 4, 6, 2, 7, 1, 0)
step_size = 0.5
MESH = pl.DeviceIdType.MESH
F32, BF16 = jnp.float32, jnp.bfloat16


def band_of(epoch):
    return epoch * BANDS // E


STRADDLERS = [
    (y, z) for y in range(NY) for z in range(NZ) if band_of((y * NZ + z) * 2) != band_of((y * NZ + z) * 2 + 1)
]


def swap(v):
    low = lax.broadcasted_iota(jnp.int32, (CUT, 128), 1) < CUT
    even = lax.rem(lax.broadcasted_iota(jnp.int32, (CUT, 128), 0), 2) == 0
    turned = pltpu.roll(v, CUT, 1)
    up = pltpu.roll(turned, CUT - 1, 0)
    down = pltpu.roll(turned, 1, 0)
    return jnp.where(low, jnp.where(even, v, down), jnp.where(even, up, v))


def finish(models_h, terms_h, terms2_h, counts_h, updated_h, models, terms, terms2, counts, updated, sems):
    loads = [
        pltpu.make_async_copy(src, dst, sems.at[i])
        for i, (src, dst) in enumerate(
            (
                (terms_h.at[pl.ds(0, 16)], terms.at[pl.ds(0, 16)]),
                (terms_h.at[pl.ds(16, 16)], terms.at[pl.ds(16, 16)]),
                (terms2_h, terms2),
                (models_h, models),
                (counts_h, counts),
            )
        )
    ]
    for load in loads:
        load.start()
    for load in loads:
        load.wait()
    even = lax.rem(lax.broadcasted_iota(jnp.int32, (CUT, 128), 0), 2) == 0
    seen_by = jnp.where(even, counts[0, 0].astype(F32), counts[0, 1].astype(F32))
    factor = step_size / seen_by
    for c in range(BANDS):
        total = jnp.zeros((CUT, 128), F32)
        for yy in range(NY):
            for zz in range(NZ):
                if band_of((yy * NZ + zz) * 2) == c:
                    total = total + terms[zz * NY + yy].astype(F32)
        for i, (ys, zs) in enumerate(STRADDLERS):
            if band_of((ys * NZ + zs) * 2 + 1) == c:
                total = total + terms2[i].astype(F32)
        updated[c] = models[c] - factor * swap(total)
        pltpu.make_async_copy(updated.at[c], updated_h.at[c], sems.at[5]).start()
    pltpu.make_async_copy(updated, updated_h, sems.at[5]).wait()


def kernel(
    models_h, obs_hbm, weights_h, coverage_h, offs_h, psf_y_h, res_y_h, psf_x_h, res_x_h, term_in, term_in2,
    models, weights, coverage, offs, psf_y, res_y, psf_x, res_x, obs_v, obs_st, obs_in, models_low, mod_in, term_out, term_out2,
    mats, mats_in, tab_a, tab_at, tab_r, fold, rows_f, wide, spread,
    scale_v, scale_in, offs_in, off_own, off_par, sc_own, sc_par,
    in_s, in_r, in2_s, obs_s, obs_r, t_s, t_r, t2_s, t2_r, small_s, small_r, local, home_sem,
):
    me = lax.axis_index("epoch")
    x = lax.rem(me, 2)
    z = lax.rem(lax.div(me, 2), NZ)
    y = lax.div(me, 2 * NZ)
    partner = me + 1 - 2 * x

    def device(yy, zz):
        return (yy * NZ + zz) * 2 + x

    def place(ky, kz):
        return lax.rem(y + ky, NY), lax.rem(z + kz, NZ)

    relative = [(ky, kz) for kz in ORDER for ky in KY]
    others = [r for r in relative if r != (0, 0)]

    def remote(src, dst, send, recv, target):
        return pltpu.make_async_remote_copy(
            src_ref=src, dst_ref=dst, send_sem=send, recv_sem=recv, device_id={"epoch": target}, device_id_type=MESH
        )

    barrier = pltpu.get_barrier_semaphore()
    pl.semaphore_signal(barrier, inc=1, device_id={"epoch": partner}, device_id_type=MESH)
    for ky, kz in others:
        pl.semaphore_signal(barrier, inc=1, device_id={"epoch": device(*place(ky, kz))}, device_id_type=MESH)

    mat_loads = [
        pltpu.make_async_copy(src, dst, local.at[6 + i])
        for i, (src, dst) in enumerate(((psf_y_h, psf_y), (res_y_h, res_y), (psf_x_h, psf_x), (res_x_h, res_x)))
    ]
    load_models = pltpu.make_async_copy(models_h, models, local.at[5])
    load_obs = pltpu.make_async_copy(obs_hbm, obs_v, local.at[0])
    load_off = pltpu.make_async_copy(offs_h, off_own, local.at[1])
    small_loads = [
        pltpu.make_async_copy(src, dst, local.at[10 + i])
        for i, (src, dst) in enumerate(
            ((weights_h, weights), (coverage_h, coverage), (offs_h, offs))
        )
    ]
    load_models.start()
    for load in mat_loads + [load_off] + small_loads:
        load.start()

    straddle = jnp.int32(0)
    straddle_id = jnp.int32(0)
    for i, (ys, zs) in enumerate(STRADDLERS):
        hit = jnp.where(jnp.logical_and(y == ys, z == zs), 1, 0).astype(jnp.int32)
        straddle = straddle + hit
        straddle_id = straddle_id + i * hit

    lane = lax.broadcasted_iota(jnp.int32, (CUT, 128), 1)
    row = lax.broadcasted_iota(jnp.int32, (CUT, 128), 0)
    low = lane < CUT
    low_half = low[:32]
    even = lax.rem(row, 2) == 0
    mask_lo = jnp.where(low, 1.0, 0.0).astype(BF16)
    mask_hi = jnp.where(low, 0.0, 1.0).astype(BF16)

    def unfold(ref):
        v = ref[...].astype(F32)
        for k in range(32):
            fold[k : k + 1, :] = v[:, k * 128 : (k + 1) * 128]
        top = fold[...]
        return top, pltpu.roll(top, CUT, 1)

    def natural(ref):
        top, bottom = unfold(ref)
        rows_f[pl.ds(0, 32, stride=2), :] = top
        rows_f[pl.ds(1, 32, stride=2), :] = bottom
        return rows_f[...]

    def doubled(v):
        return jnp.where(low, v, pltpu.roll(v, CUT, 1))

    load_models.wait()
    load_obs.start()
    for c in range(BANDS):
        models_low[c] = swap(models[c]).astype(BF16)

    def tables(slot, source):
        left = source[0].astype(F32)
        right = source[1].astype(F32)
        wide[...] = jnp.concatenate([left, left], axis=0).T

        def one(d, carry):
            tab_a[slot, d] = pltpu.roll(left, d, 1).astype(BF16)
            tab_at[slot, d] = wide[pl.ds(CUT - d, CUT), :].astype(BF16)
            tab_r[slot, d] = pltpu.roll(right, d, 1).astype(BF16)
            return carry

        lax.fori_loop(0, CUT, one, 0, unroll=4)

    pl.semaphore_wait(barrier, 32)

    def turn(g):
        kz = jnp.int32(ORDER[0])
        for i in range(1, NZ):
            kz = jnp.where(g == i, ORDER[i], kz)
        return kz

    def model_copy(ky, kz):
        yy, zz = place(ky, kz)
        band = lax.div((yy * NZ + zz) * 2 * BANDS, E)
        return remote(
            models_low.at[band], mod_in.at[0, z * NY + y], in_s, in_r.at[z], device(yy, zz)
        )

    for i, (ys, zs) in enumerate(STRADDLERS):
        band = band_of((ys * NZ + zs) * 2 + 1)
        here = jnp.logical_and(y == ys, z == zs)

        @pl.when(jnp.logical_not(here))
        def _():
            remote(
                models_low.at[band], mod_in.at[1, z * NY + y], in2_s.at[i], in_r.at[z], device(ys, zs)
            ).start()

        @pl.when(here)
        def _():
            mod_in[1, z * NY + y] = models_low[band]

    for ky, kz in others:
        model_copy(ky, kz).start()

    mod_in[0, z * NY + y] = models_low[lax.div((y * NZ + z) * 2 * BANDS, E)]

    for load in mat_loads:
        load.wait()
    top, bottom = unfold(psf_y)
    first = jnp.concatenate([top, bottom], axis=0)[:, :CUT].astype(BF16)
    second = doubled(natural(res_y)).astype(BF16)
    mats[0] = jnp.dot(first, second, preferred_element_type=F32).astype(BF16)
    first = natural(psf_x)[:, :CUT].astype(BF16)
    second = doubled(natural(res_x)).astype(BF16)
    mats[1] = jnp.dot(first, second, preferred_element_type=F32).astype(BF16)

    for load in small_loads:
        load.wait()
    scale_v[...] = weights[...] * coverage[...].astype(F32)
    send_mats = remote(mats, mats_in, small_s.at[0], small_r.at[0], partner)
    send_off = remote(offs, offs_in, small_s.at[1], small_r.at[1], partner)
    send_scale = remote(scale_v, scale_in, small_s.at[2], small_r.at[2], partner)
    send_mats.start()
    send_off.start()
    send_scale.start()
    load_scale = pltpu.make_async_copy(scale_v, sc_own, local.at[2])
    load_scale.start()

    load_obs.wait()

    def relayout(z2):
        def rows(yy, carry):
            spread[...] = obs_v[yy * 4 + z2].astype(F32)
            for s in range(4):
                f0 = spread[pl.ds(2 * s, 32, stride=8), :]
                f1 = spread[pl.ds(2 * s + 1, 32, stride=8), :]
                top = jnp.where(low_half, f0, pltpu.roll(f1, CUT, 1))
                bottom = jnp.where(low_half, pltpu.roll(f0, CUT, 1), f1)
                obs_st[s % 2, 2 * z2 + s // 2, yy] = jnp.concatenate([top, bottom], axis=0).astype(BF16)
            return carry

        lax.fori_loop(0, NY, rows, 0)

    def obs_copy(g):
        zz = lax.rem(z + turn(g), NZ)
        return remote(obs_st.at[1 - x, zz], obs_in.at[zz], obs_s, obs_r.at[g], partner)

    for z2 in range(4):
        relayout(z2)
    for g in range(NZ):
        obs_copy(jnp.int32(g)).start()

    tables(0, mats)
    send_mats.wait_recv()
    tables(1, mats_in)
    send_off.wait_recv()
    send_scale.wait_recv()
    load_off.wait()
    load_scale.wait()
    load_off = pltpu.make_async_copy(offs_in, off_par, local.at[3])
    load_scale = pltpu.make_async_copy(scale_in, sc_par, local.at[4])
    load_off.start()
    load_scale.start()
    load_off.wait()
    load_scale.wait()

    slot_own = straddle * x
    slot_par = straddle * (1 - x)
    own_first = slot_own == 0
    par_first = slot_par == 0
    offsets = (off_own, off_par)
    scales = (sc_own, sc_par)

    def term_copy(yy, zz):
        return remote(
            term_out.at[zz * NY + yy], term_in.at[z * NY + y], t_s, t_r, device(yy, zz)
        )

    def term2_copy(yy, zz):
        return remote(
            term_out2.at[zz * NY + yy], term_in2.at[straddle_id], t2_s, t2_r.at[straddle_id], device(yy, zz)
        )

    def arrived(tiles, semaphore):
        pltpu.make_async_copy(tiles, tiles, semaphore).wait()

    def split(v):
        return jnp.concatenate([v * mask_lo, v * mask_hi], axis=0)

    def group(g, carry):
        kz = turn(g)
        home = kz == 0
        zz = lax.rem(z + kz, NZ)
        obs_copy(g).wait_recv()

        def arrive(count):
            tiles = pl.ds(zz * NY, count)
            pl.when(straddle == 0)(lambda: arrived(mod_in.at[0, tiles], in_r.at[zz]))
            pl.when(straddle == 1)(lambda: arrived(mod_in.at[:, tiles], in_r.at[zz]))

        pl.when(jnp.logical_not(home))(lambda: arrive(NY))
        pl.when(home)(lambda: arrive(NY - 1))
        units = []
        for ky in KY:
            yy = lax.rem(y + ky, NY)
            for e in range(2):
                units.append((yy, e))
        state = []
        for yy, e in units:
            b = 2 * ((yy * NZ + zz) * 2 + x)
            dy0, dx0 = offsets[e][0, b], offsets[e][1, b]
            dy1, dx1 = offsets[e][0, b + 1], offsets[e][1, b + 1]
            left = tab_a[e, dy0] * mask_lo + tab_a[e, dy1] * mask_hi
            image = mod_in[slot_own if e == 0 else slot_par, zz * NY + yy]
            blurred = jnp.dot(left, split(image), preferred_element_type=F32).astype(BF16)
            state.append([yy, e, b, dy0, dy1, dx0, dx1, blurred])
        for s in state:
            yy, e, b, dy0, dy1, dx0, dx1, blurred = s
            right = jnp.concatenate([tab_r[e, dx0] * mask_lo, tab_r[e, dx1] * mask_hi], axis=0)
            predicted = lax.dot_general(blurred, right, (((1,), (1,)), ((), ())), preferred_element_type=F32)
            seen = (obs_st[x, zz, yy] if e == 0 else obs_in[zz, yy]).astype(F32)
            scale = jnp.where(low[:1], scales[e][0, b], scales[e][0, b + 1])
            s.append((scale * (predicted - seen)).astype(BF16))
        for s in state:
            yy, e, b, dy0, dy1, dx0, dx1, blurred, misfit = s
            left_t = tab_at[e, dy0] * mask_lo + tab_at[e, dy1] * mask_hi
            s.append(jnp.dot(left_t, split(misfit), preferred_element_type=F32).astype(BF16))
        terms = {}
        for s in state:
            yy, e, b, dy0, dy1, dx0, dx1, blurred, misfit, back = s
            right = jnp.concatenate([tab_r[e, dx0] * mask_lo, tab_r[e, dx1] * mask_hi], axis=0)
            terms.setdefault(len(terms) if e == 0 else len(terms) - 1, [yy]).append(
                jnp.dot(back, right, preferred_element_type=F32)
            )
        for yy, own, par in terms.values():
            zero = jnp.zeros_like(own)
            term_out[zz * NY + yy] = (jnp.where(own_first, own, zero) + jnp.where(par_first, par, zero)).astype(BF16)
            term_out2[zz * NY + yy] = (jnp.where(own_first, zero, own) + jnp.where(par_first, zero, par)).astype(BF16)
        for ky in KY:
            yy = lax.rem(y + ky, NY)

            def ship():
                term_copy(yy, zz).start()

                @pl.when(straddle == 1)
                def _():
                    term2_copy(yy, zz).start()

            if ky == 0:
                pl.when(jnp.logical_not(home))(ship)
            else:
                ship()
        return carry

    lax.fori_loop(0, 8, group, 0)

    home = z * NY + y
    pltpu.make_async_copy(term_out.at[home], term_in.at[home], home_sem.at[0]).start()

    @pl.when(straddle == 1)
    def _():
        pltpu.make_async_copy(term_out2.at[home], term_in2.at[straddle_id], home_sem.at[1]).start()

    send_mats.wait_send()
    send_off.wait_send()
    send_scale.wait_send()
    arrived(obs_in, obs_s)
    arrived(mod_in.at[0, pl.ds(0, 31)], in_s)
    for i, (ys, zs) in enumerate(STRADDLERS):

        @pl.when(jnp.logical_not(jnp.logical_and(y == ys, z == zs)))
        def _():
            arrived(models_low.at[0], in2_s.at[i])

    arrived(term_in.at[pl.ds(0, 31)], t_r)
    for i, (ys, zs) in enumerate(STRADDLERS):

        @pl.when(jnp.logical_not(jnp.logical_and(y == ys, z == zs)))
        def _():
            arrived(term_in2.at[i], t2_r.at[i])

    arrived(term_in.at[0], home_sem.at[0])
    arrived(term_out.at[pl.ds(0, 31)], t_s)

    @pl.when(straddle == 1)
    def _():
        arrived(term_out2.at[pl.ds(0, 31)], t2_s)
        arrived(term_in2.at[0], home_sem.at[1])


def on_device(
    models, observed, weights, coverage, offsets, counts, psf_y, resample_y, psf_x, resample_x
):
    pair_models = models[0].reshape(2, BANDS, 32, 128).transpose(1, 2, 0, 3).reshape(BANDS, CUT, 128)
    blocks = observed[0].reshape(16, 8, 32, 128).transpose(0, 2, 1, 3).reshape(16, 256, 128)
    anywhere = pl.BlockSpec(memory_space=pl.ANY)
    dma = pltpu.SemaphoreType.DMA
    terms, terms2 = pl.pallas_call(
        kernel,
        out_shape=(
            jax.ShapeDtypeStruct((NZ * NY, CUT, 128), BF16),
            jax.ShapeDtypeStruct((len(STRADDLERS), CUT, 128), BF16),
        ),
        in_specs=[anywhere] * 9,
        out_specs=(anywhere, anywhere),
        scratch_shapes=[
            pltpu.VMEM((BANDS, CUT, 128), F32),
            pltpu.VMEM((1, 128), F32),
            pltpu.VMEM((1, 128), jnp.int32),
            pltpu.VMEM((2, 128), jnp.int32),
            pltpu.VMEM((1, PIX2), BF16),
            pltpu.VMEM((1, PIX2), BF16),
            pltpu.VMEM((1, PIX2), BF16),
            pltpu.VMEM((1, PIX2), BF16),
            pltpu.VMEM((16, 256, 128), BF16),
            pltpu.VMEM((2, NZ, NY, CUT, 128), BF16),
            pltpu.VMEM((NZ, NY, CUT, 128), BF16),
            pltpu.VMEM((BANDS, CUT, 128), BF16),
            pltpu.VMEM((2, NZ * NY, CUT, 128), BF16),
            pltpu.VMEM((NZ * NY, CUT, 128), BF16),
            pltpu.VMEM((NZ * NY, CUT, 128), BF16),
            pltpu.VMEM((2, CUT, 128), BF16),
            pltpu.VMEM((2, CUT, 128), BF16),
            pltpu.VMEM((2, CUT, CUT, 128), BF16),
            pltpu.VMEM((2, CUT, CUT, 128), BF16),
            pltpu.VMEM((2, CUT, CUT, 128), BF16),
            pltpu.VMEM((32, 128), F32),
            pltpu.VMEM((CUT, 128), F32),
            pltpu.VMEM((128, 128), F32),
            pltpu.VMEM((256, 128), F32),
            pltpu.VMEM((1, 128), F32),
            pltpu.VMEM((1, 128), F32),
            pltpu.VMEM((2, 128), jnp.int32),
            pltpu.SMEM((2, 128), jnp.int32),
            pltpu.SMEM((2, 128), jnp.int32),
            pltpu.SMEM((1, 128), F32),
            pltpu.SMEM((1, 128), F32),
            dma, dma((NZ,)), dma((2,)), dma, dma((NZ,)),
            dma, dma, dma, dma((2,)), dma((3,)), dma((3,)), dma((13,)), dma((2,)),
        ],
        compiler_params=pltpu.CompilerParams(
            collective_id=0, has_side_effects=True, vmem_limit_bytes=60_000_000
        ),
    )(
        pair_models, blocks, weights, coverage, offsets[0].T, psf_y, resample_y, psf_x, resample_x
    )
    updated = pl.pallas_call(
        finish,
        out_shape=jax.ShapeDtypeStruct((BANDS, CUT, 128), F32),
        in_specs=[anywhere] * 4,
        out_specs=anywhere,
        scratch_shapes=[
            pltpu.VMEM((BANDS, CUT, 128), F32),
            pltpu.VMEM((NZ * NY, CUT, 128), BF16),
            pltpu.VMEM((len(STRADDLERS), CUT, 128), BF16),
            pltpu.SMEM((1, 2), jnp.int32),
            pltpu.VMEM((BANDS, CUT, 128), F32),
            dma((6,)),
        ],
        compiler_params=pltpu.CompilerParams(vmem_limit_bytes=60_000_000),
    )(pair_models, terms, terms2, counts)
    return updated.reshape(BANDS, 32, 2, 128).transpose(2, 0, 1, 3).reshape(1, 2, BANDS, PIX2)


def solution(mesh):
    return jax.shard_map(
        on_device,
        mesh=mesh,
        in_specs=(
            P("blend", "epoch", None, None),
            P("epoch", "blend", None),
            P("epoch", "blend"),
            P("epoch", "blend"),
            P("epoch", "blend", None),
            P("blend", "epoch"),
            P("epoch", None),
            P("epoch", None),
            P("epoch", None),
            P("epoch", None),
        ),
        out_specs=P("blend", "epoch", None, None),
        check_vma=False,
    )
```
